256 devices in a mesh: row: 16 (over z, y_hi), col: 16 (over y_lo, x, core).
Axes of the slice: x: 4, y: 4 (y_hi: 2, y_lo: 2; y = y_hi * 2 + y_lo), z: 8, core: 2. Of those that a mesh axis runs over, the one named last changes fastest.
Arguments:
- object_slab: float32 [2, 5120, 5120], P(None, 'row', 'col'), may hold values from -5 to 5
- probe_field: float32 [2, 512, 512], replicated, may hold values from -5 to 5
- offsets: int32 [16, 16, 1, 2], P('row', 'col'), may hold values from 0 to 64
- counts: int32 [16, 16, 1, 512, 512], P('row', 'col'), may hold values from 0 to 399
Outputs:
- updated: float32 [2, 5120, 5120], P(None, 'row', 'col')
The draws below stay inside these ranges and needn't reach their ends.
Inputs may be any that keep to these rules, and one draw needn't show every extreme that they name: Window offsets inside the widened tile of 576 cells a side; the window never leaves it.
All inputs are finite; a program needn't handle non-finite values.
Results may differ from the reference program's by a relative error of at most 0.0003.
Values sent between devices are 32-bit elements; how exact they have to be, the bound alone decides.
A program may use at most 128 MiB of HBM per device.

```python
import math
import jax
import jax.numpy as jnp
from jax import lax

TILE = 448
OVL = 128
WIN = 512
POS_DEV = 1
TILES_R = 16
TILES_C = 16
SLAB_R = 5120
SLAB_C = 5120


def with_ends(result, stream_key, least, high):
    spot = [jax.random.randint(jax.random.fold_in(stream_key, axis), (), 0, length) for axis, length in enumerate(result.shape)]
    longest = result.shape.index(max(result.shape))
    neighbour = spot[:longest] + [(spot[longest] + 1) % result.shape[longest]] + spot[longest + 1:]
    return result.at[tuple(spot)].set(least).at[tuple(neighbour)].set(high)


def levels(rng, shape, pieces, smallest, top_value):
    def one(dim, blocks):
        heights = jax.random.uniform(jax.random.fold_in(jax.random.fold_in(rng, 6), dim), (blocks,), jnp.float32, smallest / len(pieces), top_value / len(pieces))
        return jnp.repeat(jnp.exp(heights), shape[dim] // blocks).reshape((-1,) + (1,) * (len(shape) - dim - 1))

    gain = one(*pieces[0])
    for cut in pieces[1:]:
        gain = gain * one(*cut)
    return gain


def bell_draw(key, shape, scale, most, pieces=(), held_as=jnp.bfloat16):
    entries = scale * jax.random.normal(key, shape, jnp.float32)
    if pieces:
        entries = entries * levels(key, shape, pieces, -0.22, 0.18)
    return jnp.clip(entries, -most, most).astype(held_as)


def setup_inputs(seed: int = 0) -> dict:
    key_of = jax.random.split(jax.random.key(seed), 5)
    return {
        "object_slab": bell_draw(key_of[0], (2, SLAB_R, SLAB_C), 0.7, 5.0, ((1, 16), (2, 16)), jnp.float32),
        "probe_field": bell_draw(key_of[1], (2, WIN, WIN), 1.0, 5.0, (), jnp.float32),
        "offsets": with_ends(jax.random.randint(key_of[2], (TILES_R, TILES_C, POS_DEV, 2), 0, TILE + OVL - WIN + 1), jax.random.fold_in(key_of[2], 1), 0, TILE + OVL - WIN).astype(jnp.int32),
        "counts": with_ends(jax.random.randint(key_of[3], (TILES_R, TILES_C, POS_DEV, WIN, WIN), 0, 400), jax.random.fold_in(key_of[3], 1), 0, 399).astype(jnp.int32),
    }


EPSILON = 0.01
PHOTON_SCALE = 0.01
STEP_SIZE = 0.5
REGULAR = 1.0

def matmul(left, right):
    return jnp.dot(left, right, precision=lax.Precision.HIGH, preferred_element_type=jnp.float32)

def dft_tables(length):
    indices = jnp.arange(length, dtype=jnp.int32)
    products = indices[:, None] * indices[None, :] % length
    angles = products.astype(jnp.float32) * (2.0 * math.pi / length)
    norm_factor = 1.0 / math.sqrt(length)
    return (jnp.cos(angles) * norm_factor, jnp.sin(angles) * norm_factor)

def forward(real_part, imag_part, cosine_table, sine_table):
    left_real = matmul(cosine_table, real_part) + matmul(sine_table, imag_part)
    left_imag = matmul(cosine_table, imag_part) - matmul(sine_table, real_part)
    return (matmul(left_real, cosine_table) + matmul(left_imag, sine_table), matmul(left_imag, cosine_table) - matmul(left_real, sine_table))

def inverse(real_part, imag_part, cosine_table, sine_table):
    left_real = matmul(cosine_table, real_part) - matmul(sine_table, imag_part)
    left_imag = matmul(cosine_table, imag_part) + matmul(sine_table, real_part)
    return (matmul(left_real, cosine_table) - matmul(left_imag, sine_table), matmul(left_imag, cosine_table) + matmul(left_real, sine_table))

def tile_terms(widened, probe_field, tile_counts, tile_offsets, cosine_table, sine_table):
    window = probe_field.shape[-1]
    totals = jnp.zeros((3,) + widened.shape[1:], jnp.float32)
    lighting = probe_field[0] * probe_field[0] + probe_field[1] * probe_field[1]
    for position in range(tile_counts.shape[0]):
        row_start = tile_offsets[position, 0]
        col_start = tile_offsets[position, 1]
        corner_at = (jnp.int32(0), row_start, col_start)
        patch = lax.dynamic_slice(widened, corner_at, (2, window, window))
        exit_real = probe_field[0] * patch[0] - probe_field[1] * patch[1]
        exit_imag = probe_field[0] * patch[1] + probe_field[1] * patch[0]
        far_real, far_imag = forward(exit_real, exit_imag, cosine_table, sine_table)
        modulus = jnp.sqrt(far_real * far_real + far_imag * far_imag + EPSILON)
        measured = jnp.sqrt(tile_counts[position].astype(jnp.float32) * PHOTON_SCALE)
        factor = 1.0 - measured / modulus
        back_real, back_imag = inverse(factor * far_real, factor * far_imag, cosine_table, sine_table)
        grad_real = probe_field[0] * back_real + probe_field[1] * back_imag
        grad_imag = probe_field[0] * back_imag - probe_field[1] * back_real
        contrib = jnp.stack([grad_real, grad_imag, lighting])
        current = lax.dynamic_slice(totals, corner_at, contrib.shape)
        totals = lax.dynamic_update_slice(totals, current + contrib, corner_at)
    return totals

def reference(object_slab, probe_field, offsets, counts):
    cosine_table, sine_table = dft_tables(WIN)
    block_cells = TILE - OVL
    extent = block_cells + 2 * OVL
    padded = jnp.pad(object_slab, ((0, 0), (OVL, OVL), (OVL, OVL)))
    tile_rows = offsets.shape[0]
    tile_cols = offsets.shape[1]
    flat_offsets = offsets.reshape(tile_rows * tile_cols, offsets.shape[2], 2)
    flat_counts = counts.reshape(tile_rows * tile_cols, counts.shape[2], WIN, WIN)
    numbers = jnp.arange(tile_rows * tile_cols, dtype=jnp.int32)

    def visit_tile(running, inputs):
        number, tile_offsets, tile_counts = inputs
        corner_at = (jnp.int32(0), number // tile_cols * block_cells, number % tile_cols * block_cells)
        widened = lax.dynamic_slice(padded, corner_at, (2, extent, extent))
        contrib = tile_terms(widened, probe_field, tile_counts, tile_offsets, cosine_table, sine_table)
        current = lax.dynamic_slice(running, corner_at, (3, extent, extent))
        return (lax.dynamic_update_slice(running, current + contrib, corner_at), None)
    initial = jnp.zeros((3, padded.shape[1], padded.shape[2]), jnp.float32)
    totals, unused = lax.scan(visit_tile, initial, (numbers, flat_offsets, flat_counts))
    owned = totals[:, OVL:OVL + object_slab.shape[1], OVL:OVL + object_slab.shape[2]]
    return object_slab - STEP_SIZE * owned[:2] / (owned[2] + REGULAR)
```

```python
import functools
import math

import jax
import jax.numpy as jnp
import numpy as np
from jax import lax
from jax.experimental import pallas as pl
from jax.experimental.pallas import tpu as pltpu
from jax.sharding import PartitionSpec as P

EPSILON = 0.01
PHOTON_SCALE = 0.01
STEP_SIZE = 0.5
REGULAR = 1.0

N = 512
B = 128
OWN = 320
NOWHERE = -10000.0
F32 = jnp.float32
BF16 = jnp.bfloat16
POS = (1, 2, 3, 0)


def tables():
    k = np.arange(B)[:, None]
    n = np.arange(B)[None, :]
    out = []
    for r in range(4):
        angle = 2.0 * math.pi * (((4 * k + r) * n) % N) / N
        c, s = np.cos(angle) / math.sqrt(N), np.sin(angle) / math.sqrt(N)
        out.append(np.block([[c, s], [-s, c]]))
    full = np.stack(out).astype(np.float32)
    both = np.stack([full, full.transpose(0, 2, 1)])
    high = both.astype(jnp.bfloat16)
    low = (both - high.astype(np.float32)).astype(jnp.bfloat16)
    return np.stack([high, low])


def split(x):
    high = x.astype(BF16)
    return high, (x - high.astype(F32)).astype(BF16)


def dot(a, b):
    return jnp.dot(a, b, preferred_element_type=F32)


def iota(shape, dim):
    return lax.broadcasted_iota(jnp.int32, shape, dim)


def onehot(mask):
    return jnp.where(mask, 1.0, 0.0).astype(BF16)


def roll64(x):
    return pltpu.roll(x, 64, 1)


def kernel(
    rows, cols,
    obj_hbm, probe_hbm, off_ref, counts_hbm, tab_hbm,
    out_ref,
    obj, probe, counts, tab, offs, edge, mid_up, mid_dn,
    in_edge, in_mid, in_own, in_cor,
    lum, pp, meas, light, ex, zh, zl, y, kh, kl, w, acc, g, sg, rg, s_edge, s_mid, r_edge, r_mid,
    load_sem, send_sem, recv_sem,
):
    row, col = lax.axis_index("row"), lax.axis_index("col")
    has = (row > 0, row < rows - 1, col > 0, col < cols - 1)
    peer = ({"row": row - 1}, {"row": row + 1}, {"col": col - 1}, {"col": col + 1})
    UP, DN, LF, RT = range(4)
    MESH = pl.DeviceIdType.MESH

    def load(src, dst, i):
        return pltpu.make_async_copy(src, dst, load_sem.at[i])

    loads = [
        load(obj_hbm, obj, 0),
        load(probe_hbm, probe, 1),
        load(counts_hbm.at[0, 0, 0], counts, 2),
        load(tab_hbm, tab, 3),
    ]
    for c in loads:
        c.start()

    barrier = pltpu.get_barrier_semaphore()
    for d in range(4):
        @pl.when(has[d])
        def _():
            pl.semaphore_signal(barrier, inc=1, device_id=peer[d], device_id_type=MESH)

    def message(direction, slot, src, dst):
        return pltpu.make_async_remote_copy(
            src_ref=src, dst_ref=dst,
            send_sem=send_sem.at[slot], recv_sem=recv_sem.at[slot],
            device_id=peer[direction], device_id_type=MESH,
        )

    def send(direction, slot, src, dst):
        @pl.when(has[direction])
        def _():
            message(direction, slot, src, dst).start()

    OPP = (DN, UP, RT, LF)
    plan = {
        ("off", UP): (0, offs.at[1, 1], offs.at[1, 2]),
        ("off", DN): (1, offs.at[1, 1], offs.at[1, 0]),
        ("edge", UP): (2, edge.at[:, :, 0:B], in_edge.at[1]),
        ("edge", DN): (3, edge.at[:, :, OWN - B:OWN], in_edge.at[0]),
        ("mid", UP): (4, mid_up, in_mid.at[1]),
        ("mid", DN): (5, mid_dn, in_mid.at[0]),
        ("off", LF): (6, offs.at[1], offs.at[2]),
        ("off", RT): (7, offs.at[1], offs.at[0]),
        ("own", LF): (8, edge.at[0], in_own.at[1]),
        ("own", RT): (9, edge.at[1], in_own.at[0]),
        ("cor0", LF): (10, in_edge.at[0, 0], in_cor.at[1, 0]),
        ("cor0", RT): (11, in_edge.at[0, 1], in_cor.at[0, 0]),
        ("cor1", LF): (12, in_edge.at[1, 0], in_cor.at[1, 1]),
        ("cor1", RT): (13, in_edge.at[1, 1], in_cor.at[0, 1]),
        ("gcor", LF): (14, sg.at[0, :, 0:192], rg.at[1, :, 0:192]),
        ("gcor", RT): (15, sg.at[1, :, 0:192], rg.at[0, :, 0:192]),
        ("gown", LF): (16, sg.at[0, :, 192:N], rg.at[1, :, 192:N]),
        ("gown", RT): (17, sg.at[1, :, 192:N], rg.at[0, :, 192:N]),
        ("gmid", UP): (18, s_mid.at[0], r_mid.at[1]),
        ("gmid", DN): (19, s_mid.at[1], r_mid.at[0]),
        ("gedge", UP): (20, s_edge.at[0], r_edge.at[1]),
        ("gedge", DN): (21, s_edge.at[1], r_edge.at[0]),
    }

    def go(name, direction):
        send(direction, *plan[name, direction])

    def arrive(name, side):
        slot, src, dst = plan[name, OPP[side]]

        @pl.when(has[side])
        def _():
            message(side, slot, src, dst).wait_recv()

    u, v = off_ref[0, 0, 0, 0], off_ref[0, 0, 0, 1]
    lane_row = lambda n: iota((n, B), 1)
    low_half = lane_row(64) < 64

    @pl.when(row == 0)
    def _():
        in_edge[0] = jnp.zeros(in_edge.shape[1:], F32)
        in_mid[0] = jnp.zeros(in_mid.shape[1:], F32)
        r_edge[0] = jnp.zeros(r_edge.shape[1:], F32)
        r_mid[0] = jnp.zeros(r_mid.shape[1:], F32)
        offs[1, 0] = jnp.full((8, B), NOWHERE, F32)

    @pl.when(row == rows - 1)
    def _():
        in_edge[1] = jnp.zeros(in_edge.shape[1:], F32)
        in_mid[1] = jnp.zeros(in_mid.shape[1:], F32)
        r_edge[1] = jnp.zeros(r_edge.shape[1:], F32)
        r_mid[1] = jnp.zeros(r_mid.shape[1:], F32)
        offs[1, 2] = jnp.full((8, B), NOWHERE, F32)

    @pl.when(col == 0)
    def _():
        in_own[0] = jnp.zeros(in_own.shape[1:], F32)
        in_cor[0] = jnp.zeros(in_cor.shape[1:], F32)
        rg[0] = jnp.zeros(rg.shape[1:], F32)
        offs[0] = jnp.full((3, 8, B), NOWHERE, F32)

    @pl.when(col == cols - 1)
    def _():
        in_own[1] = jnp.zeros(in_own.shape[1:], F32)
        in_cor[1] = jnp.zeros(in_cor.shape[1:], F32)
        rg[1] = jnp.zeros(rg.shape[1:], F32)
        offs[2] = jnp.full((3, 8, B), NOWHERE, F32)

    uf, vf = u.astype(F32), v.astype(F32)
    offs[1, 1] = jnp.where(iota((8, B), 0) == 0, uf, vf)

    loads[0].wait()
    def tail(rs, n, ch):
        x = obj[ch, rs:rs + n, 256:OWN]
        return jnp.concatenate([x, x], axis=1)

    for ch in range(2):
        edge[0, ch] = obj[ch, :, 0:B]
        edge[1, ch] = jnp.where(
            lane_row(OWN) < 64, roll64(obj[ch, :, B:256]), tail(0, OWN, ch)
        )
    for ref, rs in ((mid_up, 0), (mid_dn, OWN - B)):
        ref[...] = jnp.where(
            lane_row(B) < 64, obj[0, rs:rs + B, B:256], roll64(obj[1, rs:rs + B, B:256])
        )

    pl.semaphore_wait(
        barrier,
        sum(h.astype(jnp.int32) for h in has),
    )

    for name in ("off", "edge", "mid"):
        go(name, UP)
        go(name, DN)
    go("own", LF)
    go("own", RT)

    loads[1].wait()
    for q in range(4):
        rs = slice(q * B, (q + 1) * B)
        pr, pi = probe[0, rs], probe[1, rs]
        hi, lo = split(pr * pr + pi * pi)
        lum[0, rs] = hi
        lum[1, rs] = lo
    d = iota((N, N), 0) + v - ((iota((N, N), 1) + 3 * B) % N)
    right = onehot((d == 0) | (d == N))
    d = iota((N, N), 1) + u - iota((N, N), 0)
    left = onehot((d == 0) | (d == N))
    for ch in range(2):
        hi, lo = split(probe[ch])
        hi, lo = split(dot(hi, right) + dot(lo, right))
        pp[ch] = dot(left, hi) + dot(left, lo)

    arrive("off", UP)
    arrive("off", DN)
    go("off", LF)
    go("off", RT)

    loads[2].wait()
    a, b = iota((N, N), 0), iota((N, N), 1)
    order_right = onehot(a == (b % B) * 4 + b // B)
    order_left = onehot(b == (a % B) * 4 + a // B)
    hi, lo = split(counts[...].astype(F32))
    hi, lo = split(dot(hi, order_right) + dot(lo, order_right))
    meas[...] = jnp.sqrt((dot(order_left, hi) + dot(order_left, lo)) * PHOTON_SCALE)

    arrive("off", LF)
    arrive("off", RT)
    light[...] = jnp.zeros(light.shape, F32)
    row_of = ((0, B, 384, B, 448), (0, OWN, 0, N, 128), (192, B, 0, B, -192))
    col_of = ((0, B, 384, B, 448), (0, 384, 0, N, 128), (128, 256, 0, B, -192))

    def tiled(x, n):
        return x if n == B else jnp.concatenate([x] * (n // B), axis=1)

    for dc in range(3):
        c0, cn, j0, jn, cshift = col_of[dc]
        for dr in range(3):
            r0, rn, i0, im, rshift = row_of[dr]
            ou = tiled(offs[dc, dr, 0:1, :], im)
            ov = tiled(offs[dc, dr, 1:2, :], cn)
            i_row = (iota((rn, im), 1) + (i0 - r0 - rshift) - iota((rn, im), 0)).astype(F32)
            pick_row = onehot(i_row + ou == 0.0)
            i_col = (iota((jn, cn), 0) + (j0 - c0 - cshift) - iota((jn, cn), 1)).astype(F32)
            pick_col = onehot(i_col + ov == 0.0)
            part = sum(dot(pick_row, lum[h, i0:i0 + im, j0:j0 + jn]) for h in range(2))
            hi, lo = split(part)
            light[r0:r0 + rn, c0:c0 + cn] += dot(hi, pick_col) + dot(lo, pick_col)
    light[...] = STEP_SIZE / (light[...] + REGULAR)

    def put(rs, n, t, wr, wi):
        at = (slice(rs, rs + n), slice(POS[t] * B, (POS[t] + 1) * B))
        pr, pi = pp[(0,) + at], pp[(1,) + at]
        ex[(0,) + at] = pr * wr - pi * wi
        ex[(1,) + at] = pr * wi + pi * wr

    arrive("own", LF)
    arrive("own", RT)
    put(B, OWN, 1, obj[0, :, 0:B], obj[1, :, 0:B])
    put(B, OWN, 2, obj[0, :, B:256], obj[1, :, B:256])

    def side_tiles(rs, n, ends, from_left, from_right):
        half = lane_row(n) < 64
        back = [roll64(x) for x in from_right]
        put(rs, n, 3, *(jnp.where(half, e, x) for e, x in zip(ends, back)))
        put(rs, n, 0, *(jnp.where(lane_row(n) < v, x, y_) for x, y_ in zip(back, from_left)))

    side_tiles(
        B, OWN, [tail(0, OWN, ch) for ch in range(2)],
        [in_own[0, ch] for ch in range(2)], [in_own[1, ch] for ch in range(2)],
    )

    loads[3].wait()
    for side in (UP, DN):
        arrive("edge", side)
        go("cor%d" % side, LF)
        go("cor%d" % side, RT)
    arrive("mid", UP)
    arrive("mid", DN)

    groups = (0, 64, 448)
    row64 = iota((64, B), 0)

    def halo(group, get):
        if group == 0:
            return jnp.where(row64 < u, get(1, 64), get(0, 0))
        if group == 64:
            return get(0, 64)
        return get(1, 0)

    def rolled_edge(group, ch):
        return roll64(halo(group, lambda s, r: in_edge[s, 1, ch, r:r + 64]))

    for rs in groups:
        put(rs, 64, 1, *(halo(rs, lambda s, r: in_edge[s, 0, ch, r:r + 64]) for ch in range(2)))
        m = halo(rs, lambda s, r: in_mid[s, r:r + 64])
        put(rs, 64, 2, *(
            jnp.where(low_half, m if ch == 0 else roll64(m), rolled_edge(rs, ch))
            for ch in range(2)
        ))

    def fwd4(x):
        (ar, ai), (br, bi), (cr, ci), (dr_, di) = x
        er, ei, fr, fi = ar + cr, ai + ci, ar - cr, ai - ci
        gr, gi, hr, hi_ = br + dr_, bi + di, br - dr_, bi - di
        return [
            (er + gr, ei + gi), (fr + hi_, fi - hr),
            (er - gr, ei - gi), (fr - hi_, fi + hr),
        ]

    def inv4(x):
        (ar, ai), (br, bi), (cr, ci), (dr_, di) = x
        er, ei, fr, fi = ar + cr, ai + ci, ar - cr, ai - ci
        gr, gi, hr, hi_ = br + dr_, bi + di, br - dr_, bi - di
        return [
            (er + gr, ei + gi), (fr - hi_, fi + hr),
            (er - gr, ei - gi), (fr + hi_, fi - hr),
        ]

    def stage_left_in(p):
        ls = slice(p * 256, p * 256 + 256)
        z = fwd4([(ex[0, q * B:(q + 1) * B, ls], ex[1, q * B:(q + 1) * B, ls]) for q in range(4)])
        for r in range(4):
            for c in range(2):
                hi, lo = split(z[r][c])
                zh[r, c * B:(c + 1) * B, ls] = hi
                zl[r, c * B:(c + 1) * B, ls] = lo
        for r in range(4):
            y[r, :, ls] = (
                dot(tab[0, 0, r], zh[r, :, ls])
                + dot(tab[0, 0, r], zl[r, :, ls])
                + dot(tab[1, 0, r], zh[r, :, ls])
            )

    stage_left_in(1)
    for side in (UP, DN):
        arrive("cor%d" % side, LF)
        arrive("cor%d" % side, RT)
    for rs in groups:
        side_tiles(
            rs, 64, [rolled_edge(rs, ch) for ch in range(2)],
            [halo(rs, lambda s, r: in_cor[0, s, ch, r:r + 64]) for ch in range(2)],
            [halo(rs, lambda s, r: in_cor[1, s, ch, r:r + 64]) for ch in range(2)],
        )
    stage_left_in(0)

    def dot3(a_hi, a_lo, b_hi, b_lo):
        return dot(a_hi, b_hi) + dot(a_hi, b_lo) + dot(a_lo, b_hi)

    for r in range(4):
        z = fwd4([
            tuple(y[r, c * B:(c + 1) * B, POS[q] * B:(POS[q] + 1) * B] for c in range(2))
            for q in range(4)
        ])
        for s in range(4):
            for c in range(2):
                hi, lo = split(z[s][c])
                kh[s, r * B:(r + 1) * B, c * B:(c + 1) * B] = hi
                kl[s, r * B:(r + 1) * B, c * B:(c + 1) * B] = lo
    for s in range(4):
        far = dot3(kh[s], kl[s], tab[0, 1, s], tab[1, 1, s])
        fr, fi = far[:, 0:B], far[:, B:256]
        factor = 1.0 - meas[:, s * B:(s + 1) * B] * lax.rsqrt(fr * fr + fi * fi + EPSILON)
        hi, lo = split(jnp.concatenate([factor * fr, factor * fi], axis=1))
        w[s] = dot3(hi, lo, tab[0, 0, s], tab[1, 0, s])

    for r in range(4):
        rs = slice(r * B, (r + 1) * B)
        x = inv4([(w[s, rs, 0:B], w[s, rs, B:256]) for s in range(4)])
        for q in range(4):
            for c in range(2):
                hi, lo = split(x[q][c])
                zh[r, c * B:(c + 1) * B, POS[q] * B:(POS[q] + 1) * B] = hi
                zl[r, c * B:(c + 1) * B, POS[q] * B:(POS[q] + 1) * B] = lo

    def stage_left_out(p):
        ls = slice(p * 256, p * 256 + 256)
        for r in range(4):
            y[r, :, ls] = (
                dot(tab[0, 1, r], zh[r, :, ls])
                + dot(tab[0, 1, r], zl[r, :, ls])
                + dot(tab[1, 1, r], zh[r, :, ls])
            )
        x = inv4([(y[r, 0:B, ls], y[r, B:256, ls]) for r in range(4)])
        for q in range(4):
            rs = slice(q * B, (q + 1) * B)
            pr, pi = pp[0, rs, ls], pp[1, rs, ls]
            br, bi = x[q]
            g[0, rs, ls] = pr * br + pi * bi
            g[1, rs, ls] = pr * bi - pi * br

    stage_left_out(0)
    for rs, n, m in ((448, 64, 0), (0, 448, 64)):
        lanes = lane_row(n)
        for c in range(2):
            g3, g0 = g[c, rs:rs + n, 0:B], g[c, rs:rs + n, B:256]
            inner = lanes < v
            sg[0, c, m:m + n] = jnp.where(inner, 0.0, g0)
            sg[1, c, m:m + n] = roll64(jnp.where(lanes >= 64, g3, jnp.where(inner, g0, 0.0)))
    for name in ("gcor", "gown"):
        go(name, LF)
        go(name, RT)
    stage_left_out(1)

    row64f = row64.astype(F32)

    def outgoing(side, get, ou):
        if side == UP:
            return (jnp.where(row64f >= ou, get(0), 0.0), get(64))
        return (get(448), jnp.where(row64f < ou, get(0), 0.0))

    own_u = offs[1, 1, 0:1, :]

    def tile(c, rs, n, t):
        return g[c, rs:rs + n, POS[t] * B:(POS[t] + 1) * B]

    for side in (UP, DN):
        m = outgoing(
            side,
            lambda rs: jnp.where(low_half, tile(0, rs, 64, 2), roll64(tile(1, rs, 64, 2))),
            own_u,
        )
        for h in range(2):
            s_mid[side, h * 64:h * 64 + 64] = m[h]
        go("gmid", side)
    arrive("gcor", LF)
    arrive("gcor", RT)
    for side in (UP, DN):
        for c in range(2):
            mine = (
                lambda rs: tile(c, rs, 64, 1),
                lambda rs: roll64(jnp.where(low_half, tile(c, rs, 64, 3), tile(c, rs, 64, 2))),
            )
            for e in range(2):
                m = outgoing(side, mine[e], own_u)
                o = outgoing(
                    side,
                    lambda rs: rg[e, c, (rs + 64) % N:(rs + 64) % N + 64],
                    offs[2 * e, 1, 0:1, :],
                )
                for h in range(2):
                    s_edge[side, e, c, h * 64:h * 64 + 64] = m[h] + o[h]
        go("gedge", side)

    arrive("gown", LF)
    arrive("gown", RT)
    lanes = lane_row(OWN)
    for c in range(2):
        x = roll64(rg[1, c, 192:N])
        acc[c, :, 0:B] = light[:, 0:B] * (tile(c, B, OWN, 1) + rg[0, c, 192:N])
        acc[c, :, B:256] = light[:, B:256] * (
            tile(c, B, OWN, 2) + jnp.where(lanes >= 64, x, 0.0)
        )
        acc[c, :, 256:384] = light[:, 256:384] * (tile(c, B, OWN, 3) + x)
        out_ref[c, B:192, :] = acc[c, B:192, 0:OWN]

    for side, rs in ((UP, 0), (DN, 192)):
        arrive("gmid", side)
        arrive("gedge", side)
        at = slice(rs, rs + B)
        for c in range(2):
            x = roll64(r_edge[side, 1, c])
            m = r_mid[side] if c == 0 else roll64(r_mid[side])
            out_ref[c, at, 0:B] = acc[c, at, 0:B] + light[at, 0:B] * r_edge[side, 0, c]
            out_ref[c, at, B:256] = acc[c, at, B:256] + light[at, B:256] * jnp.where(
                lane_row(B) < 64, m, x
            )
            last = acc[c, at, 256:384] + light[at, 256:384] * x
            out_ref[c, at, 256:OWN] = last[:, 0:64]

    for (name, direction), (slot, src, dst) in plan.items():
        @pl.when(has[direction])
        def _():
            message(direction, slot, src, dst).wait_send()


def local(rows, cols, object_slab, probe_field, offsets, counts):
    hbm = pl.BlockSpec(memory_space=pl.ANY)
    vmem = pltpu.VMEM
    step = pl.pallas_call(
        functools.partial(kernel, rows, cols),
        out_shape=jax.ShapeDtypeStruct((2, OWN, OWN), F32),
        in_specs=[hbm, hbm, pl.BlockSpec(memory_space=pltpu.SMEM), hbm, hbm],
        out_specs=pl.BlockSpec(memory_space=pltpu.VMEM),
        scratch_shapes=[
            vmem((2, OWN, OWN), F32),
            vmem((2, N, N), F32),
            vmem((N, N), jnp.int32),
            vmem((2, 2, 4, 256, 256), BF16),
            vmem((3, 3, 8, B), F32),
            vmem((2, 2, OWN, B), F32),
            vmem((B, B), F32),
            vmem((B, B), F32),
            vmem((2, 2, 2, B, B), F32),
            vmem((2, B, B), F32),
            vmem((2, 2, OWN, B), F32),
            vmem((2, 2, 2, B, B), F32),
            vmem((2, N, N), BF16),
            vmem((2, N, N), F32),
            vmem((N, N), F32),
            vmem((OWN, 384), F32),
            vmem((2, N, N), F32),
            vmem((4, 256, N), BF16),
            vmem((4, 256, N), BF16),
            vmem((4, 256, N), F32),
            vmem((4, N, 256), BF16),
            vmem((4, N, 256), BF16),
            vmem((4, N, 256), F32),
            vmem((2, OWN, 384), F32),
            vmem((2, N, N), F32),
            vmem((2, 2, N, B), F32),
            vmem((2, 2, N, B), F32),
            vmem((2, 2, 2, B, B), F32),
            vmem((2, B, B), F32),
            vmem((2, 2, 2, B, B), F32),
            vmem((2, B, B), F32),
            pltpu.SemaphoreType.DMA((4,)),
            pltpu.SemaphoreType.DMA((22,)),
            pltpu.SemaphoreType.DMA((22,)),
        ],
        compiler_params=pltpu.CompilerParams(
            collective_id=0, has_side_effects=True, vmem_limit_bytes=56 * 1024 * 1024
        ),
        name="step",
    )
    return object_slab - step(
        object_slab, probe_field, offsets, counts, jnp.asarray(tables())
    )


def solution(mesh):
    return jax.shard_map(
        functools.partial(local, mesh.shape["row"], mesh.shape["col"]),
        mesh=mesh,
        in_specs=(
            P(None, "row", "col"),
            P(),
            P("row", "col", None, None),
            P("row", "col", None, None, None),
        ),
        out_specs=P(None, "row", "col"),
        check_vma=False,
    )
```

```python
import functools
import math

import jax
import jax.numpy as jnp
import numpy as np
from jax import lax
from jax.experimental import pallas as pl
from jax.experimental.pallas import tpu as pltpu
from jax.sharding import PartitionSpec as P

EPSILON = 0.01
PHOTON_SCALE = 0.01
STEP_SIZE = 0.5
REGULAR = 1.0

N = 512
B = 128
OWN = 320
NOWHERE = -10000.0
F32 = jnp.float32
BF16 = jnp.bfloat16
POS = (1, 2, 3, 0)


def tables():
    k = np.arange(B)[:, None]
    n = np.arange(B)[None, :]
    out = []
    for r in range(4):
        angle = 2.0 * math.pi * (((4 * k + r) * n) % N) / N
        c, s = np.cos(angle) / math.sqrt(N), np.sin(angle) / math.sqrt(N)
        out.append(np.block([[c, s], [-s, c]]))
    full = np.stack(out).astype(np.float32)
    both = np.stack([full, full.transpose(0, 2, 1)])
    high = both.astype(jnp.bfloat16)
    low = (both - high.astype(np.float32)).astype(jnp.bfloat16)
    return np.stack([high, low])


def split(x):
    high = x.astype(BF16)
    return high, (x - high.astype(F32)).astype(BF16)


def dot(a, b):
    return jnp.dot(a, b, preferred_element_type=F32)


def iota(shape, dim):
    return lax.broadcasted_iota(jnp.int32, shape, dim)


def onehot(mask):
    return jnp.where(mask, 1.0, 0.0).astype(BF16)


def roll64(x):
    return pltpu.roll(x, 64, 1)


def kernel(
    rows, cols,
    obj_hbm, probe_hbm, off_ref, counts_hbm, tab_hbm,
    out_ref,
    obj, probe, counts, tab, offs, edge, mid_up, mid_dn,
    in_edge, in_mid, in_own, in_cor, relay_in,
    lum, pp, meas, light, ex, zh, zl, y, kh, kl, w, acc, g, sg, rg, s_edge, s_mid, r_edge, r_mid,
    load_sem, send_sem, recv_sem,
):
    row, col = lax.axis_index("row"), lax.axis_index("col")
    core = lax.rem(col, 2)
    has = (row > 0, row < rows - 1, col > 0, col < cols - 1)
    peer = ({"row": row - 1}, {"row": row + 1}, {"col": col - 1}, {"col": col + 1})
    UP, DN, LF, RT = range(4)
    MESH = pl.DeviceIdType.MESH

    def load(src, dst, i):
        return pltpu.make_async_copy(src, dst, load_sem.at[i])

    loads = [
        load(obj_hbm, obj, 0),
        load(probe_hbm, probe, 1),
        load(counts_hbm.at[0, 0, 0], counts, 2),
        load(tab_hbm, tab, 3),
    ]
    for c in loads:
        c.start()

    barrier = pltpu.get_barrier_semaphore()
    for d in range(4):
        @pl.when(has[d])
        def _():
            pl.semaphore_signal(barrier, inc=1, device_id=peer[d], device_id_type=MESH)

    OPP = (DN, UP, RT, LF)
    CROSS = (8, 7)
    RELAYS = {LF: (5, 3), RT: (11, 13)}
    RELAYED = ("own0", "own1", "gown0", "gown1")
    crossers = [(col == c) for c in CROSS]
    is_relay = functools.reduce(
        jnp.logical_or, [col == c for d in (LF, RT) for c in RELAYS[d]]
    )
    @pl.when(is_relay)
    def _():
        for c in CROSS:
            pl.semaphore_signal(barrier, inc=1, device_id={"col": c}, device_id_type=MESH)

    @pl.when(functools.reduce(jnp.logical_or, crossers))
    def _():
        for c in RELAYS[LF] + RELAYS[RT]:
            pl.semaphore_signal(barrier, inc=1, device_id={"col": c}, device_id_type=MESH)

    def message(direction, slot, src, dst):
        return pltpu.make_async_remote_copy(
            src_ref=src, dst_ref=dst,
            send_sem=send_sem.at[slot], recv_sem=recv_sem.at[slot],
            device_id=peer[direction], device_id_type=MESH,
        )

    def send(direction, slot, src, dst):
        @pl.when(has[direction])
        def _():
            message(direction, slot, src, dst).start()

    plan = {
        ("off", UP): (0, offs.at[1, 1], offs.at[1, 2]),
        ("off", DN): (1, offs.at[1, 1], offs.at[1, 0]),
        ("outer", UP): (2, edge.at[core, :, 0:B], in_edge.at[1, core]),
        ("outer", DN): (3, edge.at[core, :, OWN - B:OWN], in_edge.at[0, core]),
        ("inner", UP): (28, edge.at[1 - core, :, 0:B], in_edge.at[1, 1 - core]),
        ("inner", DN): (29, edge.at[1 - core, :, OWN - B:OWN], in_edge.at[0, 1 - core]),
        ("mid", UP): (4, mid_up, in_mid.at[1]),
        ("mid", DN): (5, mid_dn, in_mid.at[0]),
        ("off", LF): (6, offs.at[1], offs.at[2]),
        ("off", RT): (7, offs.at[1], offs.at[0]),
        ("own0", LF): (8, edge.at[0, :, 0:160], in_own.at[1, :, 0:160]),
        ("own0", RT): (9, edge.at[1, :, 0:160], in_own.at[0, :, 0:160]),
        ("own1", LF): (22, edge.at[0, :, 160:OWN], in_own.at[1, :, 160:OWN]),
        ("own1", RT): (23, edge.at[1, :, 160:OWN], in_own.at[0, :, 160:OWN]),
        ("cor0", LF): (10, in_edge.at[0, 0], in_cor.at[1, 0]),
        ("cor0", RT): (11, in_edge.at[0, 1], in_cor.at[0, 0]),
        ("cor1", LF): (12, in_edge.at[1, 0], in_cor.at[1, 1]),
        ("cor1", RT): (13, in_edge.at[1, 1], in_cor.at[0, 1]),
        ("gcor", LF): (14, sg.at[0, :, 0:192], rg.at[1, :, 0:192]),
        ("gcor", RT): (15, sg.at[1, :, 0:192], rg.at[0, :, 0:192]),
        ("gown0", LF): (16, sg.at[0, :, 192:352], rg.at[1, :, 192:352]),
        ("gown0", RT): (17, sg.at[1, :, 192:352], rg.at[0, :, 192:352]),
        ("gown1", LF): (24, sg.at[0, :, 352:N], rg.at[1, :, 352:N]),
        ("gown1", RT): (25, sg.at[1, :, 352:N], rg.at[0, :, 352:N]),
        ("gmid", UP): (18, s_mid.at[0], r_mid.at[1]),
        ("gmid", DN): (19, s_mid.at[1], r_mid.at[0]),
        ("gedge", UP): (20, s_edge.at[0], r_edge.at[1]),
        ("gedge", DN): (21, s_edge.at[1], r_edge.at[0]),
    }

    def routed(name, direction):
        slot, src, dst = plan[name, direction]
        k, held, held_slot = {
            "own0": (0, relay_in.at[0], 26), "own1": (1, relay_in.at[0], 26),
            "gown0": (0, relay_in.at[1], 27), "gown1": (1, relay_in.at[1], 27),
        }[name]

        def leg(source, target, sent, received, to):
            return pltpu.make_async_remote_copy(
                src_ref=source, dst_ref=target,
                send_sem=send_sem.at[sent], recv_sem=recv_sem.at[received],
                device_id={"col": to}, device_id_type=MESH,
            )

        via, end = RELAYS[direction][k], CROSS[1 - (direction - LF)]
        return via, leg(src, held, slot, held_slot, via), leg(held, dst, held_slot, slot, end)

    def go(name, direction):
        if direction not in (LF, RT) or name not in RELAYED:
            send(direction, *plan[name, direction])
            return
        crossing = col == CROSS[direction - LF]

        @pl.when(has[direction] & jnp.logical_not(crossing))
        def _():
            message(direction, *plan[name, direction]).start()

        @pl.when(crossing)
        def _():
            routed(name, direction)[1].start()

    def pass_on(*names):
        for name in names:
            for direction in (LF, RT):
                via, first, second = routed(name, direction)

                @pl.when(col == via)
                def _():
                    first.wait_recv()
                    second.start()

    def arrive(name, side):
        slot, src, dst = plan[name, OPP[side]]

        @pl.when(has[side])
        def _():
            message(side, slot, src, dst).wait_recv()

    def corner(which, side):
        arrive(which, side)
        left = core if which == "inner" else 1 - core
        for direction, flag in ((LF, 1), (RT, 0)):
            @pl.when(has[direction] & (left == flag))
            def _():
                message(direction, *plan["cor%d" % side, direction]).start()

    u, v = off_ref[0, 0, 0, 0], off_ref[0, 0, 0, 1]
    lane_row = lambda n: iota((n, B), 1)
    low_half = lane_row(64) < 64

    @pl.when(row == 0)
    def _():
        in_edge[0] = jnp.zeros(in_edge.shape[1:], F32)
        in_mid[0] = jnp.zeros(in_mid.shape[1:], F32)
        r_edge[0] = jnp.zeros(r_edge.shape[1:], F32)
        r_mid[0] = jnp.zeros(r_mid.shape[1:], F32)
        offs[1, 0] = jnp.full((8, B), NOWHERE, F32)

    @pl.when(row == rows - 1)
    def _():
        in_edge[1] = jnp.zeros(in_edge.shape[1:], F32)
        in_mid[1] = jnp.zeros(in_mid.shape[1:], F32)
        r_edge[1] = jnp.zeros(r_edge.shape[1:], F32)
        r_mid[1] = jnp.zeros(r_mid.shape[1:], F32)
        offs[1, 2] = jnp.full((8, B), NOWHERE, F32)

    @pl.when(col == 0)
    def _():
        in_own[0] = jnp.zeros(in_own.shape[1:], F32)
        in_cor[0] = jnp.zeros(in_cor.shape[1:], F32)
        rg[0] = jnp.zeros(rg.shape[1:], F32)
        offs[0] = jnp.full((3, 8, B), NOWHERE, F32)

    @pl.when(col == cols - 1)
    def _():
        in_own[1] = jnp.zeros(in_own.shape[1:], F32)
        in_cor[1] = jnp.zeros(in_cor.shape[1:], F32)
        rg[1] = jnp.zeros(rg.shape[1:], F32)
        offs[2] = jnp.full((3, 8, B), NOWHERE, F32)

    uf, vf = u.astype(F32), v.astype(F32)
    offs[1, 1] = jnp.where(iota((8, B), 0) == 0, uf, vf)

    loads[0].wait()
    def tail(rs, n, ch):
        x = obj[ch, rs:rs + n, 256:OWN]
        return jnp.concatenate([x, x], axis=1)

    for ch in range(2):
        edge[0, ch] = obj[ch, :, 0:B]
        edge[1, ch] = jnp.where(
            lane_row(OWN) < 64, roll64(obj[ch, :, B:256]), tail(0, OWN, ch)
        )
    for ref, rs in ((mid_up, 0), (mid_dn, OWN - B)):
        ref[...] = jnp.where(
            lane_row(B) < 64, obj[0, rs:rs + B, B:256], roll64(obj[1, rs:rs + B, B:256])
        )

    pl.semaphore_wait(
        barrier,
        sum(h.astype(jnp.int32) for h in has)
        + 2 * is_relay.astype(jnp.int32)
        + 4 * sum(c.astype(jnp.int32) for c in crossers),
    )

    for name in ("off", "outer", "inner", "mid"):
        go(name, UP)
        go(name, DN)
    for name in ("own0", "own1"):
        go(name, LF)
        go(name, RT)

    loads[1].wait()
    for q in range(4):
        rs = slice(q * B, (q + 1) * B)
        pr, pi = probe[0, rs], probe[1, rs]
        hi, lo = split(pr * pr + pi * pi)
        lum[0, rs] = hi
        lum[1, rs] = lo
    d = iota((N, N), 0) + v - ((iota((N, N), 1) + 3 * B) % N)
    right = onehot((d == 0) | (d == N))
    d = iota((N, N), 1) + u - iota((N, N), 0)
    left = onehot((d == 0) | (d == N))
    for ch in range(2):
        hi, lo = split(probe[ch])
        hi, lo = split(dot(hi, right) + dot(lo, right))
        pp[ch] = dot(left, hi) + dot(left, lo)

    arrive("off", UP)
    arrive("off", DN)
    go("off", LF)
    go("off", RT)

    loads[2].wait()
    a, b = iota((N, N), 0), iota((N, N), 1)
    order_right = onehot(a == (b % B) * 4 + b // B)
    order_left = onehot(b == (a % B) * 4 + a // B)
    hi, lo = split(counts[...].astype(F32))
    hi, lo = split(dot(hi, order_right) + dot(lo, order_right))
    meas[...] = jnp.sqrt((dot(order_left, hi) + dot(order_left, lo)) * PHOTON_SCALE)

    corner("outer", UP)

    arrive("off", LF)
    arrive("off", RT)
    light[...] = jnp.zeros(light.shape, F32)
    row_of = ((0, B, 384, B, 448), (0, OWN, 0, N, 128), (192, B, 0, B, -192))
    col_of = ((0, B, 384, B, 448), (0, 384, 0, N, 128), (128, 256, 0, B, -192))

    def tiled(x, n):
        return x if n == B else jnp.concatenate([x] * (n // B), axis=1)

    for dc in range(3):
        c0, cn, j0, jn, cshift = col_of[dc]
        for dr in range(3):
            r0, rn, i0, im, rshift = row_of[dr]
            ou = tiled(offs[dc, dr, 0:1, :], im)
            ov = tiled(offs[dc, dr, 1:2, :], cn)
            i_row = (iota((rn, im), 1) + (i0 - r0 - rshift) - iota((rn, im), 0)).astype(F32)
            pick_row = onehot(i_row + ou == 0.0)
            i_col = (iota((jn, cn), 0) + (j0 - c0 - cshift) - iota((jn, cn), 1)).astype(F32)
            pick_col = onehot(i_col + ov == 0.0)
            part = sum(dot(pick_row, lum[h, i0:i0 + im, j0:j0 + jn]) for h in range(2))
            hi, lo = split(part)
            light[r0:r0 + rn, c0:c0 + cn] += dot(hi, pick_col) + dot(lo, pick_col)
    light[...] = STEP_SIZE / (light[...] + REGULAR)

    pass_on("own0", "own1")

    def put(rs, n, t, wr, wi):
        at = (slice(rs, rs + n), slice(POS[t] * B, (POS[t] + 1) * B))
        pr, pi = pp[(0,) + at], pp[(1,) + at]
        ex[(0,) + at] = pr * wr - pi * wi
        ex[(1,) + at] = pr * wi + pi * wr

    put(B, OWN, 1, obj[0, :, 0:B], obj[1, :, 0:B])
    put(B, OWN, 2, obj[0, :, B:256], obj[1, :, B:256])

    def side_tiles(rs, n, ends, from_left, from_right):
        half = lane_row(n) < 64
        back = [roll64(x) for x in from_right]
        put(rs, n, 3, *(jnp.where(half, e, x) for e, x in zip(ends, back)))
        put(rs, n, 0, *(jnp.where(lane_row(n) < v, x, y_) for x, y_ in zip(back, from_left)))

    loads[3].wait()
    corner("outer", DN)
    corner("inner", UP)
    corner("inner", DN)
    for name in ("own0", "own1"):
        arrive(name, LF)
        arrive(name, RT)
    side_tiles(
        B, OWN, [tail(0, OWN, ch) for ch in range(2)],
        [in_own[0, ch] for ch in range(2)], [in_own[1, ch] for ch in range(2)],
    )
    arrive("mid", UP)
    arrive("mid", DN)

    groups = (0, 64, 448)
    row64 = iota((64, B), 0)

    def halo(group, get):
        if group == 0:
            return jnp.where(row64 < u, get(1, 64), get(0, 0))
        if group == 64:
            return get(0, 64)
        return get(1, 0)

    def rolled_edge(group, ch):
        return roll64(halo(group, lambda s, r: in_edge[s, 1, ch, r:r + 64]))

    for rs in groups:
        put(rs, 64, 1, *(halo(rs, lambda s, r: in_edge[s, 0, ch, r:r + 64]) for ch in range(2)))
        m = halo(rs, lambda s, r: in_mid[s, r:r + 64])
        put(rs, 64, 2, *(
            jnp.where(low_half, m if ch == 0 else roll64(m), rolled_edge(rs, ch))
            for ch in range(2)
        ))

    def fwd4(x):
        (ar, ai), (br, bi), (cr, ci), (dr_, di) = x
        er, ei, fr, fi = ar + cr, ai + ci, ar - cr, ai - ci
        gr, gi, hr, hi_ = br + dr_, bi + di, br - dr_, bi - di
        return [
            (er + gr, ei + gi), (fr + hi_, fi - hr),
            (er - gr, ei - gi), (fr - hi_, fi + hr),
        ]

    def inv4(x):
        (ar, ai), (br, bi), (cr, ci), (dr_, di) = x
        er, ei, fr, fi = ar + cr, ai + ci, ar - cr, ai - ci
        gr, gi, hr, hi_ = br + dr_, bi + di, br - dr_, bi - di
        return [
            (er + gr, ei + gi), (fr - hi_, fi + hr),
            (er - gr, ei - gi), (fr + hi_, fi - hr),
        ]

    def stage_left_in(p):
        ls = slice(p * 256, p * 256 + 256)
        z = fwd4([(ex[0, q * B:(q + 1) * B, ls], ex[1, q * B:(q + 1) * B, ls]) for q in range(4)])
        for r in range(4):
            for c in range(2):
                hi, lo = split(z[r][c])
                zh[r, c * B:(c + 1) * B, ls] = hi
                zl[r, c * B:(c + 1) * B, ls] = lo
        for r in range(4):
            y[r, :, ls] = (
                dot(tab[0, 0, r], zh[r, :, ls])
                + dot(tab[0, 0, r], zl[r, :, ls])
                + dot(tab[1, 0, r], zh[r, :, ls])
            )

    stage_left_in(1)
    for side in (UP, DN):
        arrive("cor%d" % side, LF)
        arrive("cor%d" % side, RT)
    for rs in groups:
        side_tiles(
            rs, 64, [rolled_edge(rs, ch) for ch in range(2)],
            [halo(rs, lambda s, r: in_cor[0, s, ch, r:r + 64]) for ch in range(2)],
            [halo(rs, lambda s, r: in_cor[1, s, ch, r:r + 64]) for ch in range(2)],
        )
    stage_left_in(0)

    def dot3(a_hi, a_lo, b_hi, b_lo):
        return dot(a_hi, b_hi) + dot(a_hi, b_lo) + dot(a_lo, b_hi)

    for r in range(4):
        z = fwd4([
            tuple(y[r, c * B:(c + 1) * B, POS[q] * B:(POS[q] + 1) * B] for c in range(2))
            for q in range(4)
        ])
        for s in range(4):
            for c in range(2):
                hi, lo = split(z[s][c])
                kh[s, r * B:(r + 1) * B, c * B:(c + 1) * B] = hi
                kl[s, r * B:(r + 1) * B, c * B:(c + 1) * B] = lo
    for s in range(4):
        far = dot3(kh[s], kl[s], tab[0, 1, s], tab[1, 1, s])
        fr, fi = far[:, 0:B], far[:, B:256]
        factor = 1.0 - meas[:, s * B:(s + 1) * B] * lax.rsqrt(fr * fr + fi * fi + EPSILON)
        hi, lo = split(jnp.concatenate([factor * fr, factor * fi], axis=1))
        w[s] = dot3(hi, lo, tab[0, 0, s], tab[1, 0, s])

    for r in range(4):
        rs = slice(r * B, (r + 1) * B)
        x = inv4([(w[s, rs, 0:B], w[s, rs, B:256]) for s in range(4)])
        for q in range(4):
            for c in range(2):
                hi, lo = split(x[q][c])
                zh[r, c * B:(c + 1) * B, POS[q] * B:(POS[q] + 1) * B] = hi
                zl[r, c * B:(c + 1) * B, POS[q] * B:(POS[q] + 1) * B] = lo

    def stage_left_out(p):
        ls = slice(p * 256, p * 256 + 256)
        for r in range(4):
            y[r, :, ls] = (
                dot(tab[0, 1, r], zh[r, :, ls])
                + dot(tab[0, 1, r], zl[r, :, ls])
                + dot(tab[1, 1, r], zh[r, :, ls])
            )
        x = inv4([(y[r, 0:B, ls], y[r, B:256, ls]) for r in range(4)])
        for q in range(4):
            rs = slice(q * B, (q + 1) * B)
            pr, pi = pp[0, rs, ls], pp[1, rs, ls]
            br, bi = x[q]
            g[0, rs, ls] = pr * br + pi * bi
            g[1, rs, ls] = pr * bi - pi * br

    stage_left_out(0)
    for rs, n, m in ((448, 64, 0), (0, 448, 64)):
        lanes = lane_row(n)
        for c in range(2):
            g3, g0 = g[c, rs:rs + n, 0:B], g[c, rs:rs + n, B:256]
            inner = lanes < v
            sg[0, c, m:m + n] = jnp.where(inner, 0.0, g0)
            sg[1, c, m:m + n] = roll64(jnp.where(lanes >= 64, g3, jnp.where(inner, g0, 0.0)))
    for name in ("gcor", "gown0", "gown1"):
        go(name, LF)
        go(name, RT)
    stage_left_out(1)

    row64f = row64.astype(F32)

    def outgoing(side, get, ou):
        if side == UP:
            return (jnp.where(row64f >= ou, get(0), 0.0), get(64))
        return (get(448), jnp.where(row64f < ou, get(0), 0.0))

    own_u = offs[1, 1, 0:1, :]

    def tile(c, rs, n, t):
        return g[c, rs:rs + n, POS[t] * B:(POS[t] + 1) * B]

    for side in (UP, DN):
        m = outgoing(
            side,
            lambda rs: jnp.where(low_half, tile(0, rs, 64, 2), roll64(tile(1, rs, 64, 2))),
            own_u,
        )
        for h in range(2):
            s_mid[side, h * 64:h * 64 + 64] = m[h]
        go("gmid", side)
    arrive("gcor", LF)
    arrive("gcor", RT)
    for side in (UP, DN):
        for c in range(2):
            mine = (
                lambda rs: tile(c, rs, 64, 1),
                lambda rs: roll64(jnp.where(low_half, tile(c, rs, 64, 3), tile(c, rs, 64, 2))),
            )
            for e in range(2):
                m = outgoing(side, mine[e], own_u)
                o = outgoing(
                    side,
                    lambda rs: rg[e, c, (rs + 64) % N:(rs + 64) % N + 64],
                    offs[2 * e, 1, 0:1, :],
                )
                for h in range(2):
                    s_edge[side, e, c, h * 64:h * 64 + 64] = m[h] + o[h]
        go("gedge", side)

    pass_on("gown0", "gown1")

    for name in ("gown0", "gown1"):
        arrive(name, LF)
        arrive(name, RT)
    lanes = lane_row(OWN)
    for c in range(2):
        x = roll64(rg[1, c, 192:N])
        acc[c, :, 0:B] = light[:, 0:B] * (tile(c, B, OWN, 1) + rg[0, c, 192:N])
        acc[c, :, B:256] = light[:, B:256] * (
            tile(c, B, OWN, 2) + jnp.where(lanes >= 64, x, 0.0)
        )
        acc[c, :, 256:384] = light[:, 256:384] * (tile(c, B, OWN, 3) + x)
        out_ref[c, B:192, :] = acc[c, B:192, 0:OWN]

    for side, rs in ((UP, 0), (DN, 192)):
        arrive("gmid", side)
        arrive("gedge", side)
        at = slice(rs, rs + B)
        for c in range(2):
            x = roll64(r_edge[side, 1, c])
            m = r_mid[side] if c == 0 else roll64(r_mid[side])
            out_ref[c, at, 0:B] = acc[c, at, 0:B] + light[at, 0:B] * r_edge[side, 0, c]
            out_ref[c, at, B:256] = acc[c, at, B:256] + light[at, B:256] * jnp.where(
                lane_row(B) < 64, m, x
            )
            last = acc[c, at, 256:384] + light[at, 256:384] * x
            out_ref[c, at, 256:OWN] = last[:, 0:64]

    for (name, direction), (slot, src, dst) in plan.items():
        if direction in (UP, DN) or name not in RELAYED:
            @pl.when(has[direction])
            def _():
                message(direction, slot, src, dst).wait_send()
            continue
        crossing = col == CROSS[direction - LF]

        @pl.when(has[direction] & jnp.logical_not(crossing))
        def _():
            message(direction, slot, src, dst).wait_send()

        via, first, second = routed(name, direction)

        @pl.when(crossing)
        def _():
            first.wait_send()

        @pl.when(col == via)
        def _():
            second.wait_send()


def local(rows, cols, object_slab, probe_field, offsets, counts):
    hbm = pl.BlockSpec(memory_space=pl.ANY)
    vmem = pltpu.VMEM
    step = pl.pallas_call(
        functools.partial(kernel, rows, cols),
        out_shape=jax.ShapeDtypeStruct((2, OWN, OWN), F32),
        in_specs=[hbm, hbm, pl.BlockSpec(memory_space=pltpu.SMEM), hbm, hbm],
        out_specs=pl.BlockSpec(memory_space=pltpu.VMEM),
        scratch_shapes=[
            vmem((2, OWN, OWN), F32),
            vmem((2, N, N), F32),
            vmem((N, N), jnp.int32),
            vmem((2, 2, 4, 256, 256), BF16),
            vmem((3, 3, 8, B), F32),
            vmem((2, 2, OWN, B), F32),
            vmem((B, B), F32),
            vmem((B, B), F32),
            vmem((2, 2, 2, B, B), F32),
            vmem((2, B, B), F32),
            vmem((2, 2, OWN, B), F32),
            vmem((2, 2, 2, B, B), F32),
            vmem((2, 2, 160, B), F32),
            vmem((2, N, N), BF16),
            vmem((2, N, N), F32),
            vmem((N, N), F32),
            vmem((OWN, 384), F32),
            vmem((2, N, N), F32),
            vmem((4, 256, N), BF16),
            vmem((4, 256, N), BF16),
            vmem((4, 256, N), F32),
            vmem((4, N, 256), BF16),
            vmem((4, N, 256), BF16),
            vmem((4, N, 256), F32),
            vmem((2, OWN, 384), F32),
            vmem((2, N, N), F32),
            vmem((2, 2, N, B), F32),
            vmem((2, 2, N, B), F32),
            vmem((2, 2, 2, B, B), F32),
            vmem((2, B, B), F32),
            vmem((2, 2, 2, B, B), F32),
            vmem((2, B, B), F32),
            pltpu.SemaphoreType.DMA((4,)),
            pltpu.SemaphoreType.DMA((30,)),
            pltpu.SemaphoreType.DMA((30,)),
        ],
        compiler_params=pltpu.CompilerParams(
            collective_id=0, has_side_effects=True, vmem_limit_bytes=56 * 1024 * 1024
        ),
        name="step",
    )
    return object_slab - step(
        object_slab, probe_field, offsets, counts, jnp.asarray(tables())
    )


def solution(mesh):
    return jax.shard_map(
        functools.partial(local, mesh.shape["row"], mesh.shape["col"]),
        mesh=mesh,
        in_specs=(
            P(None, "row", "col"),
            P(),
            P("row", "col", None, None),
            P("row", "col", None, None, None),
        ),
        out_specs=P(None, "row", "col"),
        check_vma=False,
    )
```

```python
import functools
import math

import jax
import jax.numpy as jnp
import numpy as np
from jax import lax
from jax.experimental import pallas as pl
from jax.experimental.pallas import tpu as pltpu
from jax.sharding import PartitionSpec as P

EPSILON = 0.01
PHOTON_SCALE = 0.01
STEP_SIZE = 0.5
REGULAR = 1.0

N = 512
B = 128
OWN = 320
NOWHERE = -10000.0
F32 = jnp.float32
BF16 = jnp.bfloat16
POS = (1, 2, 3, 0)


def tables():
    k = np.arange(B)[:, None]
    n = np.arange(B)[None, :]
    out = []
    for r in range(4):
        angle = 2.0 * math.pi * (((4 * k + r) * n) % N) / N
        c, s = np.cos(angle) / math.sqrt(N), np.sin(angle) / math.sqrt(N)
        out.append(np.block([[c, s], [-s, c]]))
    full = np.stack(out).astype(np.float32)
    both = np.stack([full, full.transpose(0, 2, 1)])
    high = both.astype(jnp.bfloat16)
    low = (both - high.astype(np.float32)).astype(jnp.bfloat16)
    return np.stack([high, low])


def split(x):
    high = x.astype(BF16)
    return high, (x - high.astype(F32)).astype(BF16)


def dot(a, b):
    return jnp.dot(a, b, preferred_element_type=F32)


def iota(shape, dim):
    return lax.broadcasted_iota(jnp.int32, shape, dim)


def onehot(mask):
    return jnp.where(mask, 1.0, 0.0).astype(BF16)


def roll64(x):
    return pltpu.roll(x, 64, 1)


def kernel(
    rows, cols,
    obj_hbm, probe_hbm, off_ref, counts_hbm, tab_hbm,
    out_ref,
    obj, probe, counts, tab, offs, edge, mid_up, mid_dn,
    in_edge, in_mid, in_own, in_cor, relay_in,
    lum, pp, meas, light, ex, zh, zl, y, back, kh, kl, w, acc, g, sg, rg, s_edge, s_mid, r_edge, r_mid,
    load_sem, send_sem, recv_sem,
):
    row, col = lax.axis_index("row"), lax.axis_index("col")
    core = lax.rem(col, 2)
    has = (row > 0, row < rows - 1, col > 0, col < cols - 1)
    peer = ({"row": row - 1}, {"row": row + 1}, {"col": col - 1}, {"col": col + 1})
    UP, DN, LF, RT = range(4)
    MESH = pl.DeviceIdType.MESH

    def load(src, dst, i):
        return pltpu.make_async_copy(src, dst, load_sem.at[i])

    loads = [
        load(obj_hbm, obj, 0),
        load(probe_hbm, probe, 1),
        load(counts_hbm.at[0, 0, 0], counts, 2),
        load(tab_hbm, tab, 3),
    ]
    for c in loads:
        c.start()

    barrier = pltpu.get_barrier_semaphore()
    for d in range(4):
        @pl.when(has[d])
        def _():
            pl.semaphore_signal(barrier, inc=1, device_id=peer[d], device_id_type=MESH)

    OPP = (DN, UP, RT, LF)
    CROSS = (8, 7)
    RELAYS = {LF: (5, 3, 1), RT: (11, 13, 15)}
    OWNS, GOWN = ("own0", "own1", "own2"), ("gown0", "gown1", "gown2")
    RELAYED = OWNS + GOWN
    PARTS = (slice(0, 104), slice(104, 208), slice(208, OWN))
    GPARTS = tuple(slice(192 + p.start, 192 + p.stop) for p in PARTS)
    crossers = [(col == c) for c in CROSS]
    is_relay = functools.reduce(
        jnp.logical_or, [col == c for d in (LF, RT) for c in RELAYS[d]]
    )
    @pl.when(is_relay)
    def _():
        for c in CROSS:
            pl.semaphore_signal(barrier, inc=1, device_id={"col": c}, device_id_type=MESH)

    @pl.when(functools.reduce(jnp.logical_or, crossers))
    def _():
        for c in RELAYS[LF] + RELAYS[RT]:
            pl.semaphore_signal(barrier, inc=1, device_id={"col": c}, device_id_type=MESH)

    def message(direction, slot, src, dst):
        return pltpu.make_async_remote_copy(
            src_ref=src, dst_ref=dst,
            send_sem=send_sem.at[slot], recv_sem=recv_sem.at[slot],
            device_id=peer[direction], device_id_type=MESH,
        )

    def send(direction, slot, src, dst):
        @pl.when(has[direction])
        def _():
            message(direction, slot, src, dst).start()

    plan = {
        ("off", UP): (0, offs.at[1, 1], offs.at[1, 2]),
        ("off", DN): (1, offs.at[1, 1], offs.at[1, 0]),
        ("outer", UP): (2, edge.at[core, :, 0:B], in_edge.at[1, core]),
        ("outer", DN): (3, edge.at[core, :, OWN - B:OWN], in_edge.at[0, core]),
        ("inner", UP): (28, edge.at[1 - core, :, 0:B], in_edge.at[1, 1 - core]),
        ("inner", DN): (29, edge.at[1 - core, :, OWN - B:OWN], in_edge.at[0, 1 - core]),
        ("mid", UP): (4, mid_up, in_mid.at[1]),
        ("mid", DN): (5, mid_dn, in_mid.at[0]),
        ("off", LF): (6, offs.at[1], offs.at[2]),
        ("off", RT): (7, offs.at[1], offs.at[0]),
        **{(OWNS[k], LF): (8 + 2 * k, edge.at[0, :, p], in_own.at[1, :, p]) for k, p in enumerate(PARTS)},
        **{(OWNS[k], RT): (9 + 2 * k, edge.at[1, :, p], in_own.at[0, :, p]) for k, p in enumerate(PARTS)},
        ("cor0", LF): (16, in_edge.at[0, 0], in_cor.at[1, 0]),
        ("cor0", RT): (17, in_edge.at[0, 1], in_cor.at[0, 0]),
        ("cor1", LF): (22, in_edge.at[1, 0], in_cor.at[1, 1]),
        ("cor1", RT): (23, in_edge.at[1, 1], in_cor.at[0, 1]),
        ("gcor", LF): (24, sg.at[0, :, 0:192], rg.at[1, :, 0:192]),
        ("gcor", RT): (25, sg.at[1, :, 0:192], rg.at[0, :, 0:192]),
        **{(GOWN[k], LF): (34 + 2 * k, sg.at[0, :, p], rg.at[1, :, p]) for k, p in enumerate(GPARTS)},
        **{(GOWN[k], RT): (35 + 2 * k, sg.at[1, :, p], rg.at[0, :, p]) for k, p in enumerate(GPARTS)},
        ("gmid", UP): (18, s_mid.at[0], r_mid.at[1]),
        ("gmid", DN): (19, s_mid.at[1], r_mid.at[0]),
        ("gedge0", UP): (20, s_edge.at[0, 0], r_edge.at[1, 0]),
        ("gedge0", DN): (21, s_edge.at[1, 0], r_edge.at[0, 0]),
        ("gedge1", UP): (30, s_edge.at[0, 1], r_edge.at[1, 1]),
        ("gedge1", DN): (31, s_edge.at[1, 1], r_edge.at[0, 1]),
    }

    def routed(name, direction):
        slot, src, dst = plan[name, direction]
        k, phase = int(name[-1]), 0 if name in OWNS else 1
        held, held_slot = relay_in.at[phase, :, 0:PARTS[k].stop - PARTS[k].start], 26 + phase

        def leg(source, target, sent, received, to):
            return pltpu.make_async_remote_copy(
                src_ref=source, dst_ref=target,
                send_sem=send_sem.at[sent], recv_sem=recv_sem.at[received],
                device_id={"col": to}, device_id_type=MESH,
            )

        via, end = RELAYS[direction][k], CROSS[1 - (direction - LF)]
        return (
            via,
            lambda: leg(src, held, slot, held_slot, via),
            lambda: leg(held, dst, held_slot, slot, end),
        )

    def go(name, direction):
        if direction not in (LF, RT) or name not in RELAYED:
            send(direction, *plan[name, direction])
            return
        crossing = col == CROSS[direction - LF]

        @pl.when(has[direction] & jnp.logical_not(crossing))
        def _():
            message(direction, *plan[name, direction]).start()

        @pl.when(crossing)
        def _():
            routed(name, direction)[1]().start()

    def pass_on(*names):
        for name in names:
            for direction in (LF, RT):
                via, first, second = routed(name, direction)

                @pl.when(col == via)
                def _():
                    first().wait_recv()
                    second().start()

    def arrive(name, side):
        slot, src, dst = plan[name, OPP[side]]

        @pl.when(has[side])
        def _():
            message(side, slot, src, dst).wait_recv()

    def corner(which, side):
        arrive(which, side)
        left = core if which == "inner" else 1 - core
        for direction, flag in ((LF, 1), (RT, 0)):
            @pl.when(has[direction] & (left == flag))
            def _():
                message(direction, *plan["cor%d" % side, direction]).start()

    u, v = off_ref[0, 0, 0, 0], off_ref[0, 0, 0, 1]
    lane_row = lambda n: iota((n, B), 1)
    low_half = lane_row(64) < 64

    @pl.when(row == 0)
    def _():
        in_edge[0] = jnp.zeros(in_edge.shape[1:], F32)
        in_mid[0] = jnp.zeros(in_mid.shape[1:], F32)
        r_edge[0] = jnp.zeros(r_edge.shape[1:], F32)
        r_mid[0] = jnp.zeros(r_mid.shape[1:], F32)
        offs[1, 0] = jnp.full((8, B), NOWHERE, F32)

    @pl.when(row == rows - 1)
    def _():
        in_edge[1] = jnp.zeros(in_edge.shape[1:], F32)
        in_mid[1] = jnp.zeros(in_mid.shape[1:], F32)
        r_edge[1] = jnp.zeros(r_edge.shape[1:], F32)
        r_mid[1] = jnp.zeros(r_mid.shape[1:], F32)
        offs[1, 2] = jnp.full((8, B), NOWHERE, F32)

    @pl.when(col == 0)
    def _():
        in_own[0] = jnp.zeros(in_own.shape[1:], F32)
        in_cor[0] = jnp.zeros(in_cor.shape[1:], F32)
        rg[0] = jnp.zeros(rg.shape[1:], F32)
        offs[0] = jnp.full((3, 8, B), NOWHERE, F32)

    @pl.when(col == cols - 1)
    def _():
        in_own[1] = jnp.zeros(in_own.shape[1:], F32)
        in_cor[1] = jnp.zeros(in_cor.shape[1:], F32)
        rg[1] = jnp.zeros(rg.shape[1:], F32)
        offs[2] = jnp.full((3, 8, B), NOWHERE, F32)

    uf, vf = u.astype(F32), v.astype(F32)
    offs[1, 1] = jnp.where(iota((8, B), 0) == 0, uf, vf)

    loads[0].wait()
    def tail(rs, n, ch):
        x = obj[ch, rs:rs + n, 256:OWN]
        return jnp.concatenate([x, x], axis=1)

    for ch in range(2):
        edge[0, ch] = obj[ch, :, 0:B]
        edge[1, ch] = jnp.where(
            lane_row(OWN) < 64, roll64(obj[ch, :, B:256]), tail(0, OWN, ch)
        )
    for ref, rs in ((mid_up, 0), (mid_dn, OWN - B)):
        ref[...] = jnp.where(
            lane_row(B) < 64, obj[0, rs:rs + B, B:256], roll64(obj[1, rs:rs + B, B:256])
        )

    pl.semaphore_wait(
        barrier,
        sum(h.astype(jnp.int32) for h in has)
        + 2 * is_relay.astype(jnp.int32)
        + 6 * sum(c.astype(jnp.int32) for c in crossers),
    )

    for name in ("off", "outer", "inner", "mid"):
        go(name, UP)
        go(name, DN)
    for name in OWNS:
        go(name, LF)
        go(name, RT)

    loads[1].wait()
    for q in range(4):
        rs = slice(q * B, (q + 1) * B)
        pr, pi = probe[0, rs], probe[1, rs]
        hi, lo = split(pr * pr + pi * pi)
        lum[0, rs] = hi
        lum[1, rs] = lo
    d = iota((N, N), 0) + v - ((iota((N, N), 1) + 3 * B) % N)
    right = onehot((d == 0) | (d == N))
    d = iota((N, N), 1) + u - (iota((N, N), 0) + 448) % N
    left = onehot((d == 0) | (d == N))
    for ch in range(2):
        hi, lo = split(probe[ch])
        hi, lo = split(dot(hi, right) + dot(lo, right))
        pp[ch] = dot(left, hi) + dot(left, lo)

    arrive("off", UP)
    arrive("off", DN)
    go("off", LF)
    go("off", RT)

    loads[2].wait()
    a, b = iota((N, N), 0), iota((N, N), 1)
    order_right = onehot(a == (b % B) * 4 + b // B)
    order_left = onehot(b == (a % B) * 4 + a // B)
    hi, lo = split(counts[...].astype(F32))
    hi, lo = split(dot(hi, order_right) + dot(lo, order_right))
    meas[...] = jnp.sqrt((dot(order_left, hi) + dot(order_left, lo)) * PHOTON_SCALE)

    corner("outer", UP)

    arrive("off", LF)
    arrive("off", RT)
    light[...] = jnp.zeros(light.shape, F32)
    row_of = ((0, B, 384, B, 448), (0, OWN, 0, N, 128), (192, B, 0, B, -192))
    col_of = ((0, B, 384, B, 448), (0, 384, 0, N, 128), (128, 256, 0, B, -192))

    def tiled(x, n):
        return x if n == B else jnp.concatenate([x] * (n // B), axis=1)

    for dc in range(3):
        c0, cn, j0, jn, cshift = col_of[dc]
        for dr in range(3):
            r0, rn, i0, im, rshift = row_of[dr]
            ou = tiled(offs[dc, dr, 0:1, :], im)
            ov = tiled(offs[dc, dr, 1:2, :], cn)
            i_row = (iota((rn, im), 1) + (i0 - r0 - rshift) - iota((rn, im), 0)).astype(F32)
            pick_row = onehot(i_row + ou == 0.0)
            i_col = (iota((jn, cn), 0) + (j0 - c0 - cshift) - iota((jn, cn), 1)).astype(F32)
            pick_col = onehot(i_col + ov == 0.0)
            part = sum(dot(pick_row, lum[h, i0:i0 + im, j0:j0 + jn]) for h in range(2))
            hi, lo = split(part)
            light[r0:r0 + rn, c0:c0 + cn] += dot(hi, pick_col) + dot(lo, pick_col)
    light[...] = STEP_SIZE / (light[...] + REGULAR)

    pass_on(*OWNS)

    def fwd4(x):
        (ar, ai), (br, bi), (cr, ci), (dr_, di) = x
        er, ei, fr, fi = ar + cr, ai + ci, ar - cr, ai - ci
        gr, gi, hr, hi_ = br + dr_, bi + di, br - dr_, bi - di
        return [
            (er + gr, ei + gi), (fr + hi_, fi - hr),
            (er - gr, ei - gi), (fr - hi_, fi + hr),
        ]

    def inv4(x):
        (ar, ai), (br, bi), (cr, ci), (dr_, di) = x
        er, ei, fr, fi = ar + cr, ai + ci, ar - cr, ai - ci
        gr, gi, hr, hi_ = br + dr_, bi + di, br - dr_, bi - di
        return [
            (er + gr, ei + gi), (fr - hi_, fi + hr),
            (er - gr, ei - gi), (fr + hi_, fi - hr),
        ]

    def dot3(a_hi, a_lo, b_hi, b_lo):
        return dot(a_hi, b_hi) + dot(a_hi, b_lo) + dot(a_lo, b_hi)

    def columns_in(rs):
        z = fwd4([
            tuple(ex[c, rs, POS[q] * B:(POS[q] + 1) * B] for c in range(2)) for q in range(4)
        ])
        for f in range(4):
            for c in range(2):
                hi, lo = split(z[f][c])
                kh[f, rs, c * B:(c + 1) * B] = hi
                kl[f, rs, c * B:(c + 1) * B] = lo
        for f in range(4):
            out = dot3(kh[f, rs], kl[f, rs], tab[0, 1, f], tab[1, 1, f])
            for c in range(2):
                y[c, rs, f * B:(f + 1) * B] = out[:, c * B:(c + 1) * B]

    def columns_out(rs):
        for f in range(4):
            w[f, rs] = dot3(kh[f, rs], kl[f, rs], tab[0, 0, f], tab[1, 0, f])
        x = inv4([(w[f, rs, 0:B], w[f, rs, B:256]) for f in range(4)])
        for q in range(4):
            ls = slice(POS[q] * B, (POS[q] + 1) * B)
            pr, pi = pp[0, rs, ls], pp[1, rs, ls]
            br, bi = x[q]
            g[0, rs, ls] = pr * br + pi * bi
            g[1, rs, ls] = pr * bi - pi * br

    MARGIN, INSIDE = slice(0, 192), slice(192, N)

    def put(rs, n, t, wr, wi):
        m = (rs + 64) % N
        at = (slice(m, m + n), slice(POS[t] * B, (POS[t] + 1) * B))
        pr, pi = pp[(0,) + at], pp[(1,) + at]
        ex[(0,) + at] = pr * wr - pi * wi
        ex[(1,) + at] = pr * wi + pi * wr

    put(B, OWN, 1, obj[0, :, 0:B], obj[1, :, 0:B])
    put(B, OWN, 2, obj[0, :, B:256], obj[1, :, B:256])

    def side_tiles(rs, n, ends, from_left, from_right):
        half = lane_row(n) < 64
        back = [roll64(x) for x in from_right]
        put(rs, n, 3, *(jnp.where(half, e, x) for e, x in zip(ends, back)))
        put(rs, n, 0, *(jnp.where(lane_row(n) < v, x, y_) for x, y_ in zip(back, from_left)))

    loads[3].wait()
    corner("outer", DN)
    corner("inner", UP)
    corner("inner", DN)
    for name in OWNS:
        arrive(name, LF)
        arrive(name, RT)
    side_tiles(
        B, OWN, [tail(0, OWN, ch) for ch in range(2)],
        [in_own[0, ch] for ch in range(2)], [in_own[1, ch] for ch in range(2)],
    )
    columns_in(INSIDE)
    arrive("mid", UP)
    arrive("mid", DN)

    groups = (0, 64, 448)
    row64 = iota((64, B), 0)

    def halo(group, get):
        if group == 0:
            return jnp.where(row64 < u, get(1, 64), get(0, 0))
        if group == 64:
            return get(0, 64)
        return get(1, 0)

    def rolled_edge(group, ch):
        return roll64(halo(group, lambda s, r: in_edge[s, 1, ch, r:r + 64]))

    for rs in groups:
        put(rs, 64, 1, *(halo(rs, lambda s, r: in_edge[s, 0, ch, r:r + 64]) for ch in range(2)))
        m = halo(rs, lambda s, r: in_mid[s, r:r + 64])
        put(rs, 64, 2, *(
            jnp.where(low_half, m if ch == 0 else roll64(m), rolled_edge(rs, ch))
            for ch in range(2)
        ))

    for side in (UP, DN):
        arrive("cor%d" % side, LF)
        arrive("cor%d" % side, RT)
    for rs in groups:
        side_tiles(
            rs, 64, [rolled_edge(rs, ch) for ch in range(2)],
            [halo(rs, lambda s, r: in_cor[0, s, ch, r:r + 64]) for ch in range(2)],
            [halo(rs, lambda s, r: in_cor[1, s, ch, r:r + 64]) for ch in range(2)],
        )
    columns_in(MARGIN)

    def block(ref, c, q):
        if q < 3:
            return ref[c, 64 + q * B:64 + (q + 1) * B]
        return jnp.concatenate([ref[c, 448:N], ref[c, 0:64]], axis=0)

    z = fwd4([tuple(block(y, c, q) for c in range(2)) for q in range(4)])
    for r in range(4):
        for c in range(2):
            hi, lo = split(z[r][c])
            zh[r, c * B:(c + 1) * B] = hi
            zl[r, c * B:(c + 1) * B] = lo
    for r in range(4):
        far = dot3(tab[0, 0, r], tab[1, 0, r], zh[r], zl[r])
        fr, fi = far[0:B], far[B:256]
        factor = 1.0 - meas[r * B:(r + 1) * B] * lax.rsqrt(fr * fr + fi * fi + EPSILON)
        hi, lo = split(jnp.concatenate([factor * fr, factor * fi], axis=0))
        back[r] = dot3(tab[0, 1, r], tab[1, 1, r], hi, lo)
    x = inv4([(back[r, 0:B], back[r, B:256]) for r in range(4)])
    for q in range(4):
        for c in range(2):
            parts = split(x[q][c])
            for f in range(4):
                for ref, part in zip((kh, kl), parts):
                    piece = part[:, f * B:(f + 1) * B]
                    at = slice(c * B, (c + 1) * B)
                    if q < 3:
                        ref[f, 64 + q * B:64 + (q + 1) * B, at] = piece
                    else:
                        ref[f, 448:N, at] = piece[0:64]
                        ref[f, 0:64, at] = piece[64:B]

    def to_sides(rs):
        lanes = lane_row(rs.stop - rs.start)
        inner = lanes < v
        for c in range(2):
            g3, g0 = g[c, rs, 0:B], g[c, rs, B:256]
            sg[0, c, rs] = jnp.where(inner, 0.0, g0)
            sg[1, c, rs] = roll64(jnp.where(lanes >= 64, g3, jnp.where(inner, g0, 0.0)))

    columns_out(MARGIN)
    to_sides(MARGIN)
    go("gcor", LF)
    go("gcor", RT)

    row64f = row64.astype(F32)

    def outgoing(side, get, ou):
        if side == UP:
            return (jnp.where(row64f >= ou, get(0), 0.0), get(64))
        return (get(448), jnp.where(row64f < ou, get(0), 0.0))

    own_u = offs[1, 1, 0:1, :]

    def tile(c, rs, n, t):
        m = (rs + 64) % N
        return g[c, m:m + n, POS[t] * B:(POS[t] + 1) * B]

    for side in (UP, DN):
        m = outgoing(
            side,
            lambda rs: jnp.where(low_half, tile(0, rs, 64, 2), roll64(tile(1, rs, 64, 2))),
            own_u,
        )
        for h in range(2):
            s_mid[side, h * 64:h * 64 + 64] = m[h]
        go("gmid", side)

    columns_out(INSIDE)
    to_sides(INSIDE)
    for name in GOWN:
        go(name, LF)
        go(name, RT)

    def edges(e):
        arrive("gcor", LF if e == 0 else RT)
        for side in (UP, DN):
            for c in range(2):
                if e == 0:
                    mine = lambda rs: tile(c, rs, 64, 1)
                else:
                    mine = lambda rs: roll64(
                        jnp.where(low_half, tile(c, rs, 64, 3), tile(c, rs, 64, 2))
                    )
                m = outgoing(side, mine, own_u)
                o = outgoing(
                    side,
                    lambda rs: rg[e, c, (rs + 64) % N:(rs + 64) % N + 64],
                    offs[2 * e, 1, 0:1, :],
                )
                for h in range(2):
                    s_edge[side, e, c, h * 64:h * 64 + 64] = m[h] + o[h]
            go("gedge%d" % e, side)

    for which in ("ginner", "gouter"):
        for e in range(2):
            @pl.when(core == (1 - e if which == "ginner" else e))
            def _():
                edges(e)

    pass_on(*GOWN)

    for name in GOWN:
        arrive(name, LF)
        arrive(name, RT)
    lanes = lane_row(OWN)
    for c in range(2):
        x = roll64(rg[1, c, 192:N])
        acc[c, :, 0:B] = light[:, 0:B] * (tile(c, B, OWN, 1) + rg[0, c, 192:N])
        acc[c, :, B:256] = light[:, B:256] * (
            tile(c, B, OWN, 2) + jnp.where(lanes >= 64, x, 0.0)
        )
        acc[c, :, 256:384] = light[:, 256:384] * (tile(c, B, OWN, 3) + x)
        out_ref[c, B:192, :] = acc[c, B:192, 0:OWN]

    for side, rs in ((UP, 0), (DN, 192)):
        arrive("gmid", side)
        arrive("gedge0", side)
        arrive("gedge1", side)
        at = slice(rs, rs + B)
        for c in range(2):
            x = roll64(r_edge[side, 1, c])
            m = r_mid[side] if c == 0 else roll64(r_mid[side])
            out_ref[c, at, 0:B] = acc[c, at, 0:B] + light[at, 0:B] * r_edge[side, 0, c]
            out_ref[c, at, B:256] = acc[c, at, B:256] + light[at, B:256] * jnp.where(
                lane_row(B) < 64, m, x
            )
            last = acc[c, at, 256:384] + light[at, 256:384] * x
            out_ref[c, at, 256:OWN] = last[:, 0:64]

    for (name, direction), (slot, src, dst) in plan.items():
        if direction in (UP, DN) or name not in RELAYED:
            @pl.when(has[direction])
            def _():
                message(direction, slot, src, dst).wait_send()
            continue
        crossing = col == CROSS[direction - LF]

        @pl.when(has[direction] & jnp.logical_not(crossing))
        def _():
            message(direction, slot, src, dst).wait_send()

        via, first, second = routed(name, direction)

        @pl.when(crossing)
        def _():
            first().wait_send()

        @pl.when(col == via)
        def _():
            second().wait_send()


def local(rows, cols, object_slab, probe_field, offsets, counts):
    hbm = pl.BlockSpec(memory_space=pl.ANY)
    vmem = pltpu.VMEM
    step = pl.pallas_call(
        functools.partial(kernel, rows, cols),
        out_shape=pltpu.VMEM((2, OWN, OWN), F32),
        in_specs=[hbm, hbm, pl.BlockSpec(memory_space=pltpu.SMEM), hbm, hbm],
        out_specs=pl.BlockSpec(memory_space=pltpu.VMEM),
        scratch_shapes=[
            vmem((2, OWN, OWN), F32),
            vmem((2, N, N), F32),
            vmem((N, N), jnp.int32),
            vmem((2, 2, 4, 256, 256), BF16),
            vmem((3, 3, 8, B), F32),
            vmem((2, 2, OWN, B), F32),
            vmem((B, B), F32),
            vmem((B, B), F32),
            vmem((2, 2, 2, B, B), F32),
            vmem((2, B, B), F32),
            vmem((2, 2, OWN, B), F32),
            vmem((2, 2, 2, B, B), F32),
            vmem((2, 2, 112, B), F32),
            vmem((2, N, N), BF16),
            vmem((2, N, N), F32),
            vmem((N, N), F32),
            vmem((OWN, 384), F32),
            vmem((2, N, N), F32),
            vmem((4, 256, N), BF16),
            vmem((4, 256, N), BF16),
            vmem((2, N, N), F32),
            vmem((4, 256, N), F32),
            vmem((4, N, 256), BF16),
            vmem((4, N, 256), BF16),
            vmem((4, N, 256), F32),
            vmem((2, OWN, 384), F32),
            vmem((2, N, N), F32),
            vmem((2, 2, N, B), F32),
            vmem((2, 2, N, B), F32),
            vmem((2, 2, 2, B, B), F32),
            vmem((2, B, B), F32),
            vmem((2, 2, 2, B, B), F32),
            vmem((2, B, B), F32),
            pltpu.SemaphoreType.DMA((4,)),
            pltpu.SemaphoreType.DMA((40,)),
            pltpu.SemaphoreType.DMA((40,)),
        ],
        compiler_params=pltpu.CompilerParams(
            collective_id=0, has_side_effects=True, vmem_limit_bytes=56 * 1024 * 1024
        ),
        name="step",
    )
    return object_slab - step(
        object_slab, probe_field, offsets, counts, jnp.asarray(tables())
    )


def solution(mesh):
    return jax.shard_map(
        functools.partial(local, mesh.shape["row"], mesh.shape["col"]),
        mesh=mesh,
        in_specs=(
            P(None, "row", "col"),
            P(),
            P("row", "col", None, None),
            P("row", "col", None, None, None),
        ),
        out_specs=P(None, "row", "col"),
        check_vma=False,
    )
```

```python
import functools
import math

import jax
import jax.numpy as jnp
import numpy as np
from jax import lax
from jax.experimental import pallas as pl
from jax.experimental.pallas import tpu as pltpu
from jax.sharding import PartitionSpec as P

EPSILON = 0.01
PHOTON_SCALE = 0.01
STEP_SIZE = 0.5
REGULAR = 1.0

N = 512
B = 128
OWN = 320
NOWHERE = -10000.0
F32 = jnp.float32
BF16 = jnp.bfloat16
POS = (1, 2, 3, 0)


def tables():
    k = np.arange(B)[:, None]
    n = np.arange(B)[None, :]
    out = []
    for r in range(4):
        angle = 2.0 * math.pi * (((4 * k + r) * n) % N) / N
        c, s = np.cos(angle) / math.sqrt(N), np.sin(angle) / math.sqrt(N)
        out.append(np.block([[c, s], [-s, c]]))
    full = np.stack(out).astype(np.float32)
    both = np.stack([full, full.transpose(0, 2, 1)])
    high = both.astype(jnp.bfloat16)
    low = (both - high.astype(np.float32)).astype(jnp.bfloat16)
    return np.stack([high, low])


def split(x):
    high = x.astype(BF16)
    return high, (x - high.astype(F32)).astype(BF16)


def dot(a, b):
    return jnp.dot(a, b, preferred_element_type=F32)


def iota(shape, dim):
    return lax.broadcasted_iota(jnp.int32, shape, dim)


def onehot(mask):
    return jnp.where(mask, 1.0, 0.0).astype(BF16)


def roll64(x):
    return pltpu.roll(x, 64, 1)


def kernel(
    rows, cols,
    obj_hbm, probe_hbm, off_hbm, counts_hbm, tab_hbm,
    out_ref,
    off_ref, obj, probe, counts, tab, offs, edge, mid_up, mid_dn,
    in_edge, in_mid, in_own, in_cor, relay_in,
    lum, pp, meas, light, ex, zh, zl, y, back, kh, kl, w, acc, g, sg, rg, s_edge, s_mid, r_edge, r_mid,
    load_sem, send_sem, recv_sem,
):
    row, col = lax.axis_index("row"), lax.axis_index("col")
    core = lax.rem(col, 2)
    has = (row > 0, row < rows - 1, col > 0, col < cols - 1)
    peer = ({"row": row - 1}, {"row": row + 1}, {"col": col - 1}, {"col": col + 1})
    UP, DN, LF, RT = range(4)
    MESH = pl.DeviceIdType.MESH

    def load(src, dst, i):
        return pltpu.make_async_copy(src, dst, load_sem.at[i])

    loads = [
        load(obj_hbm, obj, 0),
        load(probe_hbm, probe, 1),
        load(counts_hbm.at[0, 0, 0], counts, 2),
        load(tab_hbm, tab, 3),
        load(off_hbm, off_ref, 4),
    ]
    for c in loads:
        c.start()

    barrier = pltpu.get_barrier_semaphore()
    for d in range(4):
        @pl.when(has[d])
        def _():
            pl.semaphore_signal(barrier, inc=1, device_id=peer[d], device_id_type=MESH)

    OPP = (DN, UP, RT, LF)
    CROSS = (8, 7)
    RELAYS = {LF: (5, 3, 1), RT: (11, 13, 15)}
    OWNS, GOWN = ("own0", "own1"), ("gown0", "gown1", "gown2")
    RELAYED = OWNS + ("cor0",) + GOWN
    PARTS = (slice(0, 160), slice(160, OWN))
    GPARTS = (slice(192, 296), slice(296, 400), slice(400, N))
    crossers = [(col == c) for c in CROSS]
    is_relay = functools.reduce(
        jnp.logical_or, [col == c for d in (LF, RT) for c in RELAYS[d]]
    )
    @pl.when(is_relay)
    def _():
        for c in CROSS:
            pl.semaphore_signal(barrier, inc=1, device_id={"col": c}, device_id_type=MESH)

    @pl.when(functools.reduce(jnp.logical_or, crossers))
    def _():
        for c in RELAYS[LF] + RELAYS[RT]:
            pl.semaphore_signal(barrier, inc=1, device_id={"col": c}, device_id_type=MESH)

    def message(direction, slot, src, dst):
        return pltpu.make_async_remote_copy(
            src_ref=src, dst_ref=dst,
            send_sem=send_sem.at[slot], recv_sem=recv_sem.at[slot],
            device_id=peer[direction], device_id_type=MESH,
        )

    def send(direction, slot, src, dst):
        @pl.when(has[direction])
        def _():
            message(direction, slot, src, dst).start()

    plan = {
        ("off", UP): (0, offs.at[1, 1], offs.at[1, 2]),
        ("off", DN): (1, offs.at[1, 1], offs.at[1, 0]),
        ("outer", UP): (2, edge.at[core, :, 0:B], in_edge.at[1, core]),
        ("outer", DN): (3, edge.at[core, :, OWN - B:OWN], in_edge.at[0, core]),
        ("inner", UP): (28, edge.at[1 - core, :, 0:B], in_edge.at[1, 1 - core]),
        ("inner", DN): (29, edge.at[1 - core, :, OWN - B:OWN], in_edge.at[0, 1 - core]),
        ("mid", UP): (4, mid_up, in_mid.at[1]),
        ("mid", DN): (5, mid_dn, in_mid.at[0]),
        ("off", LF): (6, offs.at[1], offs.at[2]),
        ("off", RT): (7, offs.at[1], offs.at[0]),
        **{(OWNS[k], LF): (8 + 2 * k, edge.at[0, :, p], in_own.at[1, :, p]) for k, p in enumerate(PARTS)},
        **{(OWNS[k], RT): (9 + 2 * k, edge.at[1, :, p], in_own.at[0, :, p]) for k, p in enumerate(PARTS)},
        ("cor0", LF): (16, in_edge.at[0, 0], in_cor.at[1, 0]),
        ("cor0", RT): (17, in_edge.at[0, 1], in_cor.at[0, 0]),
        ("cor1", LF): (22, in_edge.at[1, 0], in_cor.at[1, 1]),
        ("cor1", RT): (23, in_edge.at[1, 1], in_cor.at[0, 1]),
        ("gcor", LF): (24, sg.at[0, :, 0:192], rg.at[1, :, 0:192]),
        ("gcor", RT): (25, sg.at[1, :, 0:192], rg.at[0, :, 0:192]),
        **{(GOWN[k], LF): (34 + 2 * k, sg.at[0, :, p], rg.at[1, :, p]) for k, p in enumerate(GPARTS)},
        **{(GOWN[k], RT): (35 + 2 * k, sg.at[1, :, p], rg.at[0, :, p]) for k, p in enumerate(GPARTS)},
        ("gmid", UP): (18, s_mid.at[0], r_mid.at[1]),
        ("gmid", DN): (19, s_mid.at[1], r_mid.at[0]),
        ("gedge0", UP): (20, s_edge.at[0, 0], r_edge.at[1, 0]),
        ("gedge0", DN): (21, s_edge.at[1, 0], r_edge.at[0, 0]),
        ("gedge1", UP): (30, s_edge.at[0, 1], r_edge.at[1, 1]),
        ("gedge1", DN): (31, s_edge.at[1, 1], r_edge.at[0, 1]),
    }

    def routed(name, direction):
        slot, src, dst = plan[name, direction]
        k, phase = 2 if name == "cor0" else int(name[-1]), 0 if name[0] != "g" else 1
        held, held_slot = relay_in.at[phase, :, 0:src.shape[-2]], 26 + phase

        def leg(source, target, sent, received, to):
            return pltpu.make_async_remote_copy(
                src_ref=source, dst_ref=target,
                send_sem=send_sem.at[sent], recv_sem=recv_sem.at[received],
                device_id={"col": to}, device_id_type=MESH,
            )

        via, end = RELAYS[direction][k], CROSS[1 - (direction - LF)]
        return (
            via,
            lambda: leg(src, held, slot, held_slot, via),
            lambda: leg(held, dst, held_slot, slot, end),
        )

    def go(name, direction):
        if direction not in (LF, RT) or name not in RELAYED:
            send(direction, *plan[name, direction])
            return
        crossing = col == CROSS[direction - LF]

        @pl.when(has[direction] & jnp.logical_not(crossing))
        def _():
            message(direction, *plan[name, direction]).start()

        @pl.when(crossing)
        def _():
            routed(name, direction)[1]().start()

    def gone(name, direction):
        @pl.when(has[direction])
        def _():
            message(direction, *plan[name, direction]).wait_send()

    def pass_on(*names):
        for name in names:
            for direction in (LF, RT):
                via, first, second = routed(name, direction)

                @pl.when(col == via)
                def _():
                    first().wait_recv()
                    second().start()

    def arrive(name, side):
        slot, src, dst = plan[name, OPP[side]]

        @pl.when(has[side])
        def _():
            message(side, slot, src, dst).wait_recv()

    def corner(which, side):
        arrive(which, side)
        left = core if which == "inner" else 1 - core
        for direction, flag in ((LF, 1), (RT, 0)):
            @pl.when(left == flag)
            def _():
                go("cor%d" % side, direction)

    lane_row = lambda n: iota((n, B), 1)
    low_half = lane_row(64) < 64

    @pl.when(row == 0)
    def _():
        in_edge[0] = jnp.zeros(in_edge.shape[1:], F32)
        in_mid[0] = jnp.zeros(in_mid.shape[1:], F32)
        r_edge[0] = jnp.zeros(r_edge.shape[1:], F32)
        r_mid[0] = jnp.zeros(r_mid.shape[1:], F32)
        offs[1, 0] = jnp.full((8, B), NOWHERE, F32)

    @pl.when(row == rows - 1)
    def _():
        in_edge[1] = jnp.zeros(in_edge.shape[1:], F32)
        in_mid[1] = jnp.zeros(in_mid.shape[1:], F32)
        r_edge[1] = jnp.zeros(r_edge.shape[1:], F32)
        r_mid[1] = jnp.zeros(r_mid.shape[1:], F32)
        offs[1, 2] = jnp.full((8, B), NOWHERE, F32)

    @pl.when(col == 0)
    def _():
        in_own[0] = jnp.zeros(in_own.shape[1:], F32)
        in_cor[0] = jnp.zeros(in_cor.shape[1:], F32)
        rg[0] = jnp.zeros(rg.shape[1:], F32)
        offs[0] = jnp.full((3, 8, B), NOWHERE, F32)

    @pl.when(col == cols - 1)
    def _():
        in_own[1] = jnp.zeros(in_own.shape[1:], F32)
        in_cor[1] = jnp.zeros(in_cor.shape[1:], F32)
        rg[1] = jnp.zeros(rg.shape[1:], F32)
        offs[2] = jnp.full((3, 8, B), NOWHERE, F32)

    loads[4].wait()
    u, v = off_ref[0, 0, 0, 0], off_ref[0, 0, 0, 1]
    uf, vf = u.astype(F32), v.astype(F32)
    offs[1, 1] = jnp.where(iota((8, B), 0) == 0, uf, vf)

    loads[0].wait()
    def tail(rs, n, ch):
        x = obj[ch, rs:rs + n, 256:OWN]
        return jnp.concatenate([x, x], axis=1)

    for ch in range(2):
        edge[0, ch] = obj[ch, :, 0:B]
        edge[1, ch] = jnp.where(
            lane_row(OWN) < 64, roll64(obj[ch, :, B:256]), tail(0, OWN, ch)
        )
    for ref, rs in ((mid_up, 0), (mid_dn, OWN - B)):
        ref[...] = jnp.where(
            lane_row(B) < 64, obj[0, rs:rs + B, B:256], roll64(obj[1, rs:rs + B, B:256])
        )

    pl.semaphore_wait(
        barrier,
        sum(h.astype(jnp.int32) for h in has)
        + 2 * is_relay.astype(jnp.int32)
        + 6 * sum(c.astype(jnp.int32) for c in crossers),
    )

    for name in ("off", "outer"):
        go(name, UP)
        go(name, DN)
    for name in OWNS:
        go(name, LF)
        go(name, RT)

    loads[1].wait()
    for q in range(4):
        rs = slice(q * B, (q + 1) * B)
        pr, pi = probe[0, rs], probe[1, rs]
        hi, lo = split(pr * pr + pi * pi)
        lum[0, rs] = hi
        lum[1, rs] = lo
    d = iota((N, N), 0) + v - ((iota((N, N), 1) + 3 * B) % N)
    right = onehot((d == 0) | (d == N))
    d = iota((N, N), 1) + u - (iota((N, N), 0) + 448) % N
    left = onehot((d == 0) | (d == N))
    for ch in range(2):
        hi, lo = split(probe[ch])
        hi, lo = split(dot(hi, right) + dot(lo, right))
        pp[ch] = dot(left, hi) + dot(left, lo)

    arrive("off", UP)
    arrive("off", DN)
    go("off", LF)
    go("off", RT)

    loads[2].wait()
    a, b = iota((N, N), 0), iota((N, N), 1)
    order_right = onehot(a == (b % B) * 4 + b // B)
    order_left = onehot(b == (a % B) * 4 + a // B)
    hi, lo = split(counts[...].astype(F32))
    hi, lo = split(dot(hi, order_right) + dot(lo, order_right))
    meas[...] = jnp.sqrt((dot(order_left, hi) + dot(order_left, lo)) * PHOTON_SCALE)

    for direction in (UP, DN):
        gone("outer", direction)
    go("inner", UP)
    go("inner", DN)
    corner("outer", UP)

    arrive("off", LF)
    arrive("off", RT)
    light[...] = jnp.zeros(light.shape, F32)
    row_of = ((0, B, 384, B, 448), (0, OWN, 0, N, 128), (192, B, 0, B, -192))
    col_of = ((0, B, 384, B, 448), (0, 384, 0, N, 128), (128, 256, 0, B, -192))

    def tiled(x, n):
        return x if n == B else jnp.concatenate([x] * (n // B), axis=1)

    for dc in range(3):
        c0, cn, j0, jn, cshift = col_of[dc]
        for dr in range(3):
            r0, rn, i0, im, rshift = row_of[dr]
            ou = tiled(offs[dc, dr, 0:1, :], im)
            ov = tiled(offs[dc, dr, 1:2, :], cn)
            i_row = (iota((rn, im), 1) + (i0 - r0 - rshift) - iota((rn, im), 0)).astype(F32)
            pick_row = onehot(i_row + ou == 0.0)
            i_col = (iota((jn, cn), 0) + (j0 - c0 - cshift) - iota((jn, cn), 1)).astype(F32)
            pick_col = onehot(i_col + ov == 0.0)
            part = sum(dot(pick_row, lum[h, i0:i0 + im, j0:j0 + jn]) for h in range(2))
            hi, lo = split(part)
            light[r0:r0 + rn, c0:c0 + cn] += dot(hi, pick_col) + dot(lo, pick_col)
    light[...] = STEP_SIZE / (light[...] + REGULAR)

    pass_on(*OWNS)

    def fwd4(x):
        (ar, ai), (br, bi), (cr, ci), (dr_, di) = x
        er, ei, fr, fi = ar + cr, ai + ci, ar - cr, ai - ci
        gr, gi, hr, hi_ = br + dr_, bi + di, br - dr_, bi - di
        return [
            (er + gr, ei + gi), (fr + hi_, fi - hr),
            (er - gr, ei - gi), (fr - hi_, fi + hr),
        ]

    def inv4(x):
        (ar, ai), (br, bi), (cr, ci), (dr_, di) = x
        er, ei, fr, fi = ar + cr, ai + ci, ar - cr, ai - ci
        gr, gi, hr, hi_ = br + dr_, bi + di, br - dr_, bi - di
        return [
            (er + gr, ei + gi), (fr - hi_, fi + hr),
            (er - gr, ei - gi), (fr + hi_, fi - hr),
        ]

    def dot3(a_hi, a_lo, b_hi, b_lo):
        return dot(a_hi, b_hi) + dot(a_hi, b_lo) + dot(a_lo, b_hi)

    def columns_in(rs):
        z = fwd4([
            tuple(ex[c, rs, POS[q] * B:(POS[q] + 1) * B] for c in range(2)) for q in range(4)
        ])
        for f in range(4):
            for c in range(2):
                hi, lo = split(z[f][c])
                kh[f, rs, c * B:(c + 1) * B] = hi
                kl[f, rs, c * B:(c + 1) * B] = lo
        for f in range(4):
            out = dot3(kh[f, rs], kl[f, rs], tab[0, 1, f], tab[1, 1, f])
            for c in range(2):
                y[c, rs, f * B:(f + 1) * B] = out[:, c * B:(c + 1) * B]

    def columns_out(rs):
        for f in range(4):
            w[f, rs] = dot3(kh[f, rs], kl[f, rs], tab[0, 0, f], tab[1, 0, f])
        x = inv4([(w[f, rs, 0:B], w[f, rs, B:256]) for f in range(4)])
        for q in range(4):
            ls = slice(POS[q] * B, (POS[q] + 1) * B)
            pr, pi = pp[0, rs, ls], pp[1, rs, ls]
            br, bi = x[q]
            g[0, rs, ls] = pr * br + pi * bi
            g[1, rs, ls] = pr * bi - pi * br

    MARGIN, INSIDE = slice(0, 192), slice(192, N)

    def put(rs, n, t, wr, wi):
        m = (rs + 64) % N
        at = (slice(m, m + n), slice(POS[t] * B, (POS[t] + 1) * B))
        pr, pi = pp[(0,) + at], pp[(1,) + at]
        ex[(0,) + at] = pr * wr - pi * wi
        ex[(1,) + at] = pr * wi + pi * wr

    put(B, OWN, 1, obj[0, :, 0:B], obj[1, :, 0:B])
    put(B, OWN, 2, obj[0, :, B:256], obj[1, :, B:256])

    def side_tiles(rs, n, ends, from_left, from_right):
        half = lane_row(n) < 64
        back = [roll64(x) for x in from_right]
        put(rs, n, 3, *(jnp.where(half, e, x) for e, x in zip(ends, back)))
        put(rs, n, 0, *(jnp.where(lane_row(n) < v, x, y_) for x, y_ in zip(back, from_left)))

    loads[3].wait()
    corner("outer", DN)
    pass_on("cor0")
    for direction in (UP, DN):
        gone("inner", direction)
    go("mid", UP)
    go("mid", DN)
    corner("inner", UP)
    corner("inner", DN)
    for name in OWNS:
        arrive(name, LF)
        arrive(name, RT)
    side_tiles(
        B, OWN, [tail(0, OWN, ch) for ch in range(2)],
        [in_own[0, ch] for ch in range(2)], [in_own[1, ch] for ch in range(2)],
    )
    columns_in(INSIDE)
    arrive("mid", UP)
    arrive("mid", DN)

    groups = (0, 64, 448)
    row64 = iota((64, B), 0)

    def halo(group, get):
        if group == 0:
            return jnp.where(row64 < u, get(1, 64), get(0, 0))
        if group == 64:
            return get(0, 64)
        return get(1, 0)

    def rolled_edge(group, ch):
        return roll64(halo(group, lambda s, r: in_edge[s, 1, ch, r:r + 64]))

    for rs in groups:
        put(rs, 64, 1, *(halo(rs, lambda s, r: in_edge[s, 0, ch, r:r + 64]) for ch in range(2)))
        m = halo(rs, lambda s, r: in_mid[s, r:r + 64])
        put(rs, 64, 2, *(
            jnp.where(low_half, m if ch == 0 else roll64(m), rolled_edge(rs, ch))
            for ch in range(2)
        ))

    for side in (UP, DN):
        arrive("cor%d" % side, LF)
        arrive("cor%d" % side, RT)
    for rs in groups:
        side_tiles(
            rs, 64, [rolled_edge(rs, ch) for ch in range(2)],
            [halo(rs, lambda s, r: in_cor[0, s, ch, r:r + 64]) for ch in range(2)],
            [halo(rs, lambda s, r: in_cor[1, s, ch, r:r + 64]) for ch in range(2)],
        )
    columns_in(MARGIN)

    def block(ref, c, q):
        if q < 3:
            return ref[c, 64 + q * B:64 + (q + 1) * B]
        return jnp.concatenate([ref[c, 448:N], ref[c, 0:64]], axis=0)

    z = fwd4([tuple(block(y, c, q) for c in range(2)) for q in range(4)])
    for r in range(4):
        for c in range(2):
            hi, lo = split(z[r][c])
            zh[r, c * B:(c + 1) * B] = hi
            zl[r, c * B:(c + 1) * B] = lo
    for r in range(4):
        far = dot3(tab[0, 0, r], tab[1, 0, r], zh[r], zl[r])
        fr, fi = far[0:B], far[B:256]
        factor = 1.0 - meas[r * B:(r + 1) * B] * lax.rsqrt(fr * fr + fi * fi + EPSILON)
        hi, lo = split(jnp.concatenate([factor * fr, factor * fi], axis=0))
        back[r] = dot3(tab[0, 1, r], tab[1, 1, r], hi, lo)
    x = inv4([(back[r, 0:B], back[r, B:256]) for r in range(4)])
    for q in range(4):
        for c in range(2):
            parts = split(x[q][c])
            for f in range(4):
                for ref, part in zip((kh, kl), parts):
                    piece = part[:, f * B:(f + 1) * B]
                    at = slice(c * B, (c + 1) * B)
                    if q < 3:
                        ref[f, 64 + q * B:64 + (q + 1) * B, at] = piece
                    else:
                        ref[f, 448:N, at] = piece[0:64]
                        ref[f, 0:64, at] = piece[64:B]

    def to_sides(rs):
        lanes = lane_row(rs.stop - rs.start)
        inner = lanes < v
        for c in range(2):
            g3, g0 = g[c, rs, 0:B], g[c, rs, B:256]
            sg[0, c, rs] = jnp.where(inner, 0.0, g0)
            sg[1, c, rs] = roll64(jnp.where(lanes >= 64, g3, jnp.where(inner, g0, 0.0)))

    columns_out(MARGIN)

    row64f = row64.astype(F32)

    def outgoing(side, get, ou):
        if side == UP:
            return (jnp.where(row64f >= ou, get(0), 0.0), get(64))
        return (get(448), jnp.where(row64f < ou, get(0), 0.0))

    own_u = offs[1, 1, 0:1, :]

    def tile(c, rs, n, t):
        m = (rs + 64) % N
        return g[c, m:m + n, POS[t] * B:(POS[t] + 1) * B]

    for side in (UP, DN):
        m = outgoing(
            side,
            lambda rs: jnp.where(low_half, tile(0, rs, 64, 2), roll64(tile(1, rs, 64, 2))),
            own_u,
        )
        for h in range(2):
            s_mid[side, h * 64:h * 64 + 64] = m[h]
        go("gmid", side)
    to_sides(MARGIN)
    go("gcor", LF)
    go("gcor", RT)

    columns_out(INSIDE)
    to_sides(INSIDE)
    for name in GOWN:
        go(name, LF)
        go(name, RT)

    def edges(e):
        arrive("gcor", LF if e == 0 else RT)
        for side in (UP, DN):
            for c in range(2):
                if e == 0:
                    mine = lambda rs: tile(c, rs, 64, 1)
                else:
                    mine = lambda rs: roll64(
                        jnp.where(low_half, tile(c, rs, 64, 3), tile(c, rs, 64, 2))
                    )
                m = outgoing(side, mine, own_u)
                o = outgoing(
                    side,
                    lambda rs: rg[e, c, (rs + 64) % N:(rs + 64) % N + 64],
                    offs[2 * e, 1, 0:1, :],
                )
                for h in range(2):
                    s_edge[side, e, c, h * 64:h * 64 + 64] = m[h] + o[h]
            go("gedge%d" % e, side)

    for which in ("ginner", "gouter"):
        for e in range(2):
            @pl.when(core == (1 - e if which == "ginner" else e))
            def _():
                edges(e)

    pass_on(*GOWN)

    for name in GOWN:
        arrive(name, LF)
        arrive(name, RT)
    lanes = lane_row(OWN)
    for c in range(2):
        x = roll64(rg[1, c, 192:N])
        acc[c, :, 0:B] = light[:, 0:B] * (tile(c, B, OWN, 1) + rg[0, c, 192:N])
        acc[c, :, B:256] = light[:, B:256] * (
            tile(c, B, OWN, 2) + jnp.where(lanes >= 64, x, 0.0)
        )
        acc[c, :, 256:384] = light[:, 256:384] * (tile(c, B, OWN, 3) + x)
        out_ref[c, B:192, :] = acc[c, B:192, 0:OWN]

    for side, rs in ((UP, 0), (DN, 192)):
        arrive("gmid", side)
        arrive("gedge0", side)
        arrive("gedge1", side)
        at = slice(rs, rs + B)
        for c in range(2):
            x = roll64(r_edge[side, 1, c])
            m = r_mid[side] if c == 0 else roll64(r_mid[side])
            out_ref[c, at, 0:B] = acc[c, at, 0:B] + light[at, 0:B] * r_edge[side, 0, c]
            out_ref[c, at, B:256] = acc[c, at, B:256] + light[at, B:256] * jnp.where(
                lane_row(B) < 64, m, x
            )
            last = acc[c, at, 256:384] + light[at, 256:384] * x
            out_ref[c, at, 256:OWN] = last[:, 0:64]

    for (name, direction), (slot, src, dst) in plan.items():
        if name in ("outer", "inner"):
            continue
        if direction in (UP, DN) or name not in RELAYED:
            @pl.when(has[direction])
            def _():
                message(direction, slot, src, dst).wait_send()
            continue
        crossing = col == CROSS[direction - LF]

        @pl.when(has[direction] & jnp.logical_not(crossing))
        def _():
            message(direction, slot, src, dst).wait_send()

        via, first, second = routed(name, direction)

        @pl.when(crossing)
        def _():
            first().wait_send()

        @pl.when(col == via)
        def _():
            second().wait_send()


def local(rows, cols, object_slab, probe_field, offsets, counts):
    hbm = pl.BlockSpec(memory_space=pl.ANY)
    vmem = pltpu.VMEM
    step = pl.pallas_call(
        functools.partial(kernel, rows, cols),
        out_shape=pltpu.VMEM((2, OWN, OWN), F32),
        in_specs=[hbm] * 5,
        out_specs=pl.BlockSpec(memory_space=pltpu.VMEM),
        scratch_shapes=[
            pltpu.SMEM((1, 1, 1, 2), jnp.int32),
            vmem((2, OWN, OWN), F32),
            vmem((2, N, N), F32),
            vmem((N, N), jnp.int32),
            vmem((2, 2, 4, 256, 256), BF16),
            vmem((3, 3, 8, B), F32),
            vmem((2, 2, OWN, B), F32),
            vmem((B, B), F32),
            vmem((B, B), F32),
            vmem((2, 2, 2, B, B), F32),
            vmem((2, B, B), F32),
            vmem((2, 2, OWN, B), F32),
            vmem((2, 2, 2, B, B), F32),
            vmem((2, 2, 160, B), F32),
            vmem((2, N, N), BF16),
            vmem((2, N, N), F32),
            vmem((N, N), F32),
            vmem((OWN, 384), F32),
            vmem((2, N, N), F32),
            vmem((4, 256, N), BF16),
            vmem((4, 256, N), BF16),
            vmem((2, N, N), F32),
            vmem((4, 256, N), F32),
            vmem((4, N, 256), BF16),
            vmem((4, N, 256), BF16),
            vmem((4, N, 256), F32),
            vmem((2, OWN, 384), F32),
            vmem((2, N, N), F32),
            vmem((2, 2, N, B), F32),
            vmem((2, 2, N, B), F32),
            vmem((2, 2, 2, B, B), F32),
            vmem((2, B, B), F32),
            vmem((2, 2, 2, B, B), F32),
            vmem((2, B, B), F32),
            pltpu.SemaphoreType.DMA((5,)),
            pltpu.SemaphoreType.DMA((40,)),
            pltpu.SemaphoreType.DMA((40,)),
        ],
        compiler_params=pltpu.CompilerParams(
            collective_id=0, has_side_effects=True, vmem_limit_bytes=56 * 1024 * 1024
        ),
        name="step",
    )
    return object_slab - step(
        object_slab, probe_field, offsets, counts, jnp.asarray(tables())
    )


def solution(mesh):
    return jax.shard_map(
        functools.partial(local, mesh.shape["row"], mesh.shape["col"]),
        mesh=mesh,
        in_specs=(
            P(None, "row", "col"),
            P(),
            P("row", "col", None, None),
            P("row", "col", None, None, None),
        ),
        out_specs=P(None, "row", "col"),
        check_vma=False,
    )
```

```python
import functools
import math

import jax
import jax.numpy as jnp
import numpy as np
from jax import lax
from jax.experimental import pallas as pl
from jax.experimental.pallas import tpu as pltpu
from jax.sharding import PartitionSpec as P

EPSILON = 0.01
PHOTON_SCALE = 0.01
STEP_SIZE = 0.5
REGULAR = 1.0

N = 512
B = 128
OWN = 320
NOWHERE = -10000.0
F32 = jnp.float32
BF16 = jnp.bfloat16
POS = (1, 2, 3, 0)


def tables():
    k = np.arange(B)[:, None]
    n = np.arange(B)[None, :]
    out = []
    for r in range(4):
        angle = 2.0 * math.pi * (((4 * k + r) * n) % N) / N
        c, s = np.cos(angle) / math.sqrt(N), np.sin(angle) / math.sqrt(N)
        out.append(np.block([[c, s], [-s, c]]))
    full = np.stack(out).astype(np.float32)
    both = np.stack([full, full.transpose(0, 2, 1)])
    high = both.astype(jnp.bfloat16)
    low = (both - high.astype(np.float32)).astype(jnp.bfloat16)
    return np.stack([high, low])


def split(x):
    high = x.astype(BF16)
    return high, (x - high.astype(F32)).astype(BF16)


def dot(a, b):
    return jnp.dot(a, b, preferred_element_type=F32)


def iota(shape, dim):
    return lax.broadcasted_iota(jnp.int32, shape, dim)


def onehot(mask):
    return jnp.where(mask, 1.0, 0.0).astype(BF16)


def roll64(x):
    return pltpu.roll(x, 64, 1)


def kernel(
    rows, cols,
    obj_hbm, probe_hbm, off_hbm, counts_hbm, tab_hbm,
    out_ref,
    off_ref, obj, probe, counts, tab, offs, edge, mid_up, mid_dn,
    in_edge, in_mid, in_own, in_cor, relay_in,
    lum, pp, meas, light, ex, zh, zl, y, back, kh, kl, w, acc, g, sg, rg, s_edge, s_mid, r_edge, r_mid,
    load_sem, send_sem, recv_sem,
):
    row, col = lax.axis_index("row"), lax.axis_index("col")
    core = lax.rem(col, 2)
    has = (row > 0, row < rows - 1, col > 0, col < cols - 1)
    peer = ({"row": row - 1}, {"row": row + 1}, {"col": col - 1}, {"col": col + 1})
    UP, DN, LF, RT = range(4)
    MESH = pl.DeviceIdType.MESH

    def load(src, dst, i):
        return pltpu.make_async_copy(src, dst, load_sem.at[i])

    loads = [
        load(obj_hbm, obj, 0),
        load(probe_hbm, probe, 1),
        load(counts_hbm.at[0, 0, 0], counts, 2),
        load(tab_hbm, tab, 3),
        load(off_hbm, off_ref, 4),
    ]
    loads[0].start()
    loads[4].start()

    barrier = pltpu.get_barrier_semaphore()
    for d in range(4):
        @pl.when(has[d])
        def _():
            pl.semaphore_signal(barrier, inc=1, device_id=peer[d], device_id_type=MESH)

    OPP = (DN, UP, RT, LF)
    CROSS = (8, 7)
    RELAYS = {LF: (3, 1, 5), RT: (13, 15, 11)}
    OWNS, GOWN = ("own0", "own1"), ("gown0", "gown1", "gown2")
    RELAYED = OWNS + ("cor0",) + GOWN
    PARTS = (slice(0, 160), slice(160, OWN))
    GPARTS = (slice(192, 296), slice(296, 400), slice(400, N))
    crossers = [(col == c) for c in CROSS]
    is_relay = functools.reduce(
        jnp.logical_or, [col == c for d in (LF, RT) for c in RELAYS[d]]
    )
    @pl.when(is_relay)
    def _():
        for c in CROSS:
            pl.semaphore_signal(barrier, inc=1, device_id={"col": c}, device_id_type=MESH)

    @pl.when(functools.reduce(jnp.logical_or, crossers))
    def _():
        for c in RELAYS[LF] + RELAYS[RT]:
            pl.semaphore_signal(barrier, inc=1, device_id={"col": c}, device_id_type=MESH)

    def message(direction, slot, src, dst):
        return pltpu.make_async_remote_copy(
            src_ref=src, dst_ref=dst,
            send_sem=send_sem.at[slot], recv_sem=recv_sem.at[slot],
            device_id=peer[direction], device_id_type=MESH,
        )

    def send(direction, slot, src, dst):
        @pl.when(has[direction])
        def _():
            message(direction, slot, src, dst).start()

    plan = {
        ("off", UP): (0, offs.at[1, 1], offs.at[1, 2]),
        ("off", DN): (1, offs.at[1, 1], offs.at[1, 0]),
        ("outer", UP): (2, edge.at[core, :, 0:B], in_edge.at[1, core]),
        ("outer", DN): (3, edge.at[core, :, OWN - B:OWN], in_edge.at[0, core]),
        ("inner", UP): (28, edge.at[1 - core, :, 0:B], in_edge.at[1, 1 - core]),
        ("inner", DN): (29, edge.at[1 - core, :, OWN - B:OWN], in_edge.at[0, 1 - core]),
        ("mid", UP): (4, mid_up, in_mid.at[1]),
        ("mid", DN): (5, mid_dn, in_mid.at[0]),
        ("off", LF): (6, offs.at[1], offs.at[2]),
        ("off", RT): (7, offs.at[1], offs.at[0]),
        **{(OWNS[k], LF): (8 + 2 * k, edge.at[0, :, p], in_own.at[1, :, p]) for k, p in enumerate(PARTS)},
        **{(OWNS[k], RT): (9 + 2 * k, edge.at[1, :, p], in_own.at[0, :, p]) for k, p in enumerate(PARTS)},
        ("cor0", LF): (16, in_edge.at[0, 0], in_cor.at[1, 0]),
        ("cor0", RT): (17, in_edge.at[0, 1], in_cor.at[0, 0]),
        ("cor1", LF): (22, in_edge.at[1, 0], in_cor.at[1, 1]),
        ("cor1", RT): (23, in_edge.at[1, 1], in_cor.at[0, 1]),
        ("gcor", LF): (24, sg.at[0, :, 0:192], rg.at[1, :, 0:192]),
        ("gcor", RT): (25, sg.at[1, :, 0:192], rg.at[0, :, 0:192]),
        **{(GOWN[k], LF): (34 + 2 * k, sg.at[0, :, p], rg.at[1, :, p]) for k, p in enumerate(GPARTS)},
        **{(GOWN[k], RT): (35 + 2 * k, sg.at[1, :, p], rg.at[0, :, p]) for k, p in enumerate(GPARTS)},
        ("gmid", UP): (18, s_mid.at[0], r_mid.at[1]),
        ("gmid", DN): (19, s_mid.at[1], r_mid.at[0]),
        ("gedge0", UP): (20, s_edge.at[0, 0], r_edge.at[1, 0]),
        ("gedge0", DN): (21, s_edge.at[1, 0], r_edge.at[0, 0]),
        ("gedge1", UP): (30, s_edge.at[0, 1], r_edge.at[1, 1]),
        ("gedge1", DN): (31, s_edge.at[1, 1], r_edge.at[0, 1]),
    }

    def routed(name, direction):
        slot, src, dst = plan[name, direction]
        k, phase = 2 if name == "cor0" else int(name[-1]), 0 if name[0] != "g" else 1
        held, held_slot = relay_in.at[phase, :, 0:src.shape[-2]], 26 + phase

        def leg(source, target, sent, received, to):
            return pltpu.make_async_remote_copy(
                src_ref=source, dst_ref=target,
                send_sem=send_sem.at[sent], recv_sem=recv_sem.at[received],
                device_id={"col": to}, device_id_type=MESH,
            )

        via, end = RELAYS[direction][k], CROSS[1 - (direction - LF)]
        return (
            via,
            lambda: leg(src, held, slot, held_slot, via),
            lambda: leg(held, dst, held_slot, slot, end),
        )

    def go(name, direction):
        if direction not in (LF, RT) or name not in RELAYED:
            send(direction, *plan[name, direction])
            return
        crossing = col == CROSS[direction - LF]

        @pl.when(has[direction] & jnp.logical_not(crossing))
        def _():
            message(direction, *plan[name, direction]).start()

        @pl.when(crossing)
        def _():
            routed(name, direction)[1]().start()

    def gone(name, direction):
        @pl.when(has[direction])
        def _():
            message(direction, *plan[name, direction]).wait_send()

    def pass_on(*names):
        for name in names:
            for direction in (LF, RT):
                via, first, second = routed(name, direction)

                @pl.when(col == via)
                def _():
                    first().wait_recv()
                    second().start()

    def arrive(name, side):
        slot, src, dst = plan[name, OPP[side]]

        @pl.when(has[side])
        def _():
            message(side, slot, src, dst).wait_recv()

    def corner(which, side):
        arrive(which, side)
        left = core if which == "inner" else 1 - core
        for direction, flag in ((LF, 1), (RT, 0)):
            @pl.when(left == flag)
            def _():
                go("cor%d" % side, direction)

    lane_row = lambda n: iota((n, B), 1)
    low_half = lane_row(64) < 64

    @pl.when(row == 0)
    def _():
        in_edge[0] = jnp.zeros(in_edge.shape[1:], F32)
        in_mid[0] = jnp.zeros(in_mid.shape[1:], F32)
        r_edge[0] = jnp.zeros(r_edge.shape[1:], F32)
        r_mid[0] = jnp.zeros(r_mid.shape[1:], F32)
        offs[1, 0] = jnp.full((8, B), NOWHERE, F32)

    @pl.when(row == rows - 1)
    def _():
        in_edge[1] = jnp.zeros(in_edge.shape[1:], F32)
        in_mid[1] = jnp.zeros(in_mid.shape[1:], F32)
        r_edge[1] = jnp.zeros(r_edge.shape[1:], F32)
        r_mid[1] = jnp.zeros(r_mid.shape[1:], F32)
        offs[1, 2] = jnp.full((8, B), NOWHERE, F32)

    @pl.when(col == 0)
    def _():
        in_own[0] = jnp.zeros(in_own.shape[1:], F32)
        in_cor[0] = jnp.zeros(in_cor.shape[1:], F32)
        rg[0] = jnp.zeros(rg.shape[1:], F32)
        offs[0] = jnp.full((3, 8, B), NOWHERE, F32)

    @pl.when(col == cols - 1)
    def _():
        in_own[1] = jnp.zeros(in_own.shape[1:], F32)
        in_cor[1] = jnp.zeros(in_cor.shape[1:], F32)
        rg[1] = jnp.zeros(rg.shape[1:], F32)
        offs[2] = jnp.full((3, 8, B), NOWHERE, F32)

    loads[4].wait()
    u, v = off_ref[0, 0, 0, 0], off_ref[0, 0, 0, 1]
    uf, vf = u.astype(F32), v.astype(F32)
    offs[1, 1] = jnp.where(iota((8, B), 0) == 0, uf, vf)

    loads[0].wait()
    for c in loads[1:4]:
        c.start()
    def tail(rs, n, ch):
        x = obj[ch, rs:rs + n, 256:OWN]
        return jnp.concatenate([x, x], axis=1)

    for ch in range(2):
        edge[0, ch] = obj[ch, :, 0:B]
        edge[1, ch] = jnp.where(
            lane_row(OWN) < 64, roll64(obj[ch, :, B:256]), tail(0, OWN, ch)
        )
    for ref, rs in ((mid_up, 0), (mid_dn, OWN - B)):
        ref[...] = jnp.where(
            lane_row(B) < 64, obj[0, rs:rs + B, B:256], roll64(obj[1, rs:rs + B, B:256])
        )

    pl.semaphore_wait(
        barrier,
        sum(h.astype(jnp.int32) for h in has)
        + 2 * is_relay.astype(jnp.int32)
        + 6 * sum(c.astype(jnp.int32) for c in crossers),
    )

    for name in ("off", "outer"):
        go(name, UP)
        go(name, DN)
    for name in OWNS:
        go(name, LF)
        go(name, RT)

    loads[1].wait()
    for q in range(4):
        rs = slice(q * B, (q + 1) * B)
        pr, pi = probe[0, rs], probe[1, rs]
        hi, lo = split(pr * pr + pi * pi)
        lum[0, rs] = hi
        lum[1, rs] = lo
    d = iota((N, N), 0) + v - ((iota((N, N), 1) + 3 * B) % N)
    right = onehot((d == 0) | (d == N))
    d = iota((N, N), 1) + u - (iota((N, N), 0) + 448) % N
    left = onehot((d == 0) | (d == N))
    for ch in range(2):
        hi, lo = split(probe[ch])
        hi, lo = split(dot(hi, right) + dot(lo, right))
        pp[ch] = dot(left, hi) + dot(left, lo)

    arrive("off", UP)
    arrive("off", DN)
    go("off", LF)
    go("off", RT)

    loads[2].wait()
    a, b = iota((N, N), 0), iota((N, N), 1)
    order_right = onehot(a == (b % B) * 4 + b // B)
    order_left = onehot(b == (a % B) * 4 + a // B)
    hi, lo = split(counts[...].astype(F32))
    hi, lo = split(dot(hi, order_right) + dot(lo, order_right))
    meas[...] = jnp.sqrt((dot(order_left, hi) + dot(order_left, lo)) * PHOTON_SCALE)

    for direction in (UP, DN):
        gone("outer", direction)
    go("inner", UP)
    go("inner", DN)
    corner("outer", UP)

    arrive("off", LF)
    arrive("off", RT)
    light[...] = jnp.zeros(light.shape, F32)
    row_of = ((0, B, 384, B, 448), (0, OWN, 0, N, 128), (192, B, 0, B, -192))
    col_of = ((0, B, 384, B, 448), (0, 384, 0, N, 128), (128, 256, 0, B, -192))

    def tiled(x, n):
        return x if n == B else jnp.concatenate([x] * (n // B), axis=1)

    for dc in range(3):
        c0, cn, j0, jn, cshift = col_of[dc]
        for dr in range(3):
            r0, rn, i0, im, rshift = row_of[dr]
            ou = tiled(offs[dc, dr, 0:1, :], im)
            ov = tiled(offs[dc, dr, 1:2, :], cn)
            i_row = (iota((rn, im), 1) + (i0 - r0 - rshift) - iota((rn, im), 0)).astype(F32)
            pick_row = onehot(i_row + ou == 0.0)
            i_col = (iota((jn, cn), 0) + (j0 - c0 - cshift) - iota((jn, cn), 1)).astype(F32)
            pick_col = onehot(i_col + ov == 0.0)
            part = sum(dot(pick_row, lum[h, i0:i0 + im, j0:j0 + jn]) for h in range(2))
            hi, lo = split(part)
            light[r0:r0 + rn, c0:c0 + cn] += dot(hi, pick_col) + dot(lo, pick_col)
    light[...] = STEP_SIZE / (light[...] + REGULAR)

    pass_on(*OWNS)

    def fwd4(x):
        (ar, ai), (br, bi), (cr, ci), (dr_, di) = x
        er, ei, fr, fi = ar + cr, ai + ci, ar - cr, ai - ci
        gr, gi, hr, hi_ = br + dr_, bi + di, br - dr_, bi - di
        return [
            (er + gr, ei + gi), (fr + hi_, fi - hr),
            (er - gr, ei - gi), (fr - hi_, fi + hr),
        ]

    def inv4(x):
        (ar, ai), (br, bi), (cr, ci), (dr_, di) = x
        er, ei, fr, fi = ar + cr, ai + ci, ar - cr, ai - ci
        gr, gi, hr, hi_ = br + dr_, bi + di, br - dr_, bi - di
        return [
            (er + gr, ei + gi), (fr - hi_, fi + hr),
            (er - gr, ei - gi), (fr + hi_, fi - hr),
        ]

    def dot3(a_hi, a_lo, b_hi, b_lo):
        return dot(a_hi, b_hi) + dot(a_hi, b_lo) + dot(a_lo, b_hi)

    def columns_in(rs):
        z = fwd4([
            tuple(ex[c, rs, POS[q] * B:(POS[q] + 1) * B] for c in range(2)) for q in range(4)
        ])
        for f in range(4):
            for c in range(2):
                hi, lo = split(z[f][c])
                kh[f, rs, c * B:(c + 1) * B] = hi
                kl[f, rs, c * B:(c + 1) * B] = lo
        for f in range(4):
            out = dot3(kh[f, rs], kl[f, rs], tab[0, 1, f], tab[1, 1, f])
            for c in range(2):
                y[c, rs, f * B:(f + 1) * B] = out[:, c * B:(c + 1) * B]

    def columns_out(rs):
        for f in range(4):
            w[f, rs] = dot3(kh[f, rs], kl[f, rs], tab[0, 0, f], tab[1, 0, f])
        x = inv4([(w[f, rs, 0:B], w[f, rs, B:256]) for f in range(4)])
        for q in range(4):
            ls = slice(POS[q] * B, (POS[q] + 1) * B)
            pr, pi = pp[0, rs, ls], pp[1, rs, ls]
            br, bi = x[q]
            g[0, rs, ls] = pr * br + pi * bi
            g[1, rs, ls] = pr * bi - pi * br

    MARGIN, INSIDE = slice(0, 192), slice(192, N)

    def put(rs, n, t, wr, wi):
        m = (rs + 64) % N
        at = (slice(m, m + n), slice(POS[t] * B, (POS[t] + 1) * B))
        pr, pi = pp[(0,) + at], pp[(1,) + at]
        ex[(0,) + at] = pr * wr - pi * wi
        ex[(1,) + at] = pr * wi + pi * wr

    put(B, OWN, 1, obj[0, :, 0:B], obj[1, :, 0:B])
    put(B, OWN, 2, obj[0, :, B:256], obj[1, :, B:256])

    def side_tiles(rs, n, ends, from_left, from_right):
        half = lane_row(n) < 64
        back = [roll64(x) for x in from_right]
        put(rs, n, 3, *(jnp.where(half, e, x) for e, x in zip(ends, back)))
        put(rs, n, 0, *(jnp.where(lane_row(n) < v, x, y_) for x, y_ in zip(back, from_left)))

    loads[3].wait()
    corner("outer", DN)
    for direction in (UP, DN):
        gone("inner", direction)
    go("mid", UP)
    go("mid", DN)
    pass_on("cor0")
    corner("inner", UP)
    corner("inner", DN)
    for name in OWNS:
        arrive(name, LF)
        arrive(name, RT)
    side_tiles(
        B, OWN, [tail(0, OWN, ch) for ch in range(2)],
        [in_own[0, ch] for ch in range(2)], [in_own[1, ch] for ch in range(2)],
    )
    columns_in(INSIDE)

    groups = (0, 64, 448)
    row64 = iota((64, B), 0)

    def halo(group, get):
        if group == 0:
            return jnp.where(row64 < u, get(1, 64), get(0, 0))
        if group == 64:
            return get(0, 64)
        return get(1, 0)

    def rolled_edge(group, ch):
        return roll64(halo(group, lambda s, r: in_edge[s, 1, ch, r:r + 64]))

    for rs in groups:
        put(rs, 64, 1, *(halo(rs, lambda s, r: in_edge[s, 0, ch, r:r + 64]) for ch in range(2)))
    for side in (UP, DN):
        arrive("cor%d" % side, LF)
        arrive("cor%d" % side, RT)
    for rs in groups:
        side_tiles(
            rs, 64, [rolled_edge(rs, ch) for ch in range(2)],
            [halo(rs, lambda s, r: in_cor[0, s, ch, r:r + 64]) for ch in range(2)],
            [halo(rs, lambda s, r: in_cor[1, s, ch, r:r + 64]) for ch in range(2)],
        )
    arrive("mid", UP)
    arrive("mid", DN)
    for rs in groups:
        m = halo(rs, lambda s, r: in_mid[s, r:r + 64])
        put(rs, 64, 2, *(
            jnp.where(low_half, m if ch == 0 else roll64(m), rolled_edge(rs, ch))
            for ch in range(2)
        ))
    columns_in(MARGIN)

    def block(ref, c, q):
        if q < 3:
            return ref[c, 64 + q * B:64 + (q + 1) * B]
        return jnp.concatenate([ref[c, 448:N], ref[c, 0:64]], axis=0)

    z = fwd4([tuple(block(y, c, q) for c in range(2)) for q in range(4)])
    for r in range(4):
        for c in range(2):
            hi, lo = split(z[r][c])
            zh[r, c * B:(c + 1) * B] = hi
            zl[r, c * B:(c + 1) * B] = lo
    for r in range(4):
        far = dot3(tab[0, 0, r], tab[1, 0, r], zh[r], zl[r])
        fr, fi = far[0:B], far[B:256]
        factor = 1.0 - meas[r * B:(r + 1) * B] * lax.rsqrt(fr * fr + fi * fi + EPSILON)
        hi, lo = split(jnp.concatenate([factor * fr, factor * fi], axis=0))
        back[r] = dot3(tab[0, 1, r], tab[1, 1, r], hi, lo)
    x = inv4([(back[r, 0:B], back[r, B:256]) for r in range(4)])
    for q in range(4):
        for c in range(2):
            parts = split(x[q][c])
            for f in range(4):
                for ref, part in zip((kh, kl), parts):
                    piece = part[:, f * B:(f + 1) * B]
                    at = slice(c * B, (c + 1) * B)
                    if q < 3:
                        ref[f, 64 + q * B:64 + (q + 1) * B, at] = piece
                    else:
                        ref[f, 448:N, at] = piece[0:64]
                        ref[f, 0:64, at] = piece[64:B]

    def to_sides(rs):
        lanes = lane_row(rs.stop - rs.start)
        inner = lanes < v
        for c in range(2):
            g3, g0 = g[c, rs, 0:B], g[c, rs, B:256]
            sg[0, c, rs] = jnp.where(inner, 0.0, g0)
            sg[1, c, rs] = roll64(jnp.where(lanes >= 64, g3, jnp.where(inner, g0, 0.0)))

    columns_out(MARGIN)

    row64f = row64.astype(F32)

    def outgoing(side, get, ou):
        if side == UP:
            return (jnp.where(row64f >= ou, get(0), 0.0), get(64))
        return (get(448), jnp.where(row64f < ou, get(0), 0.0))

    own_u = offs[1, 1, 0:1, :]

    def tile(c, rs, n, t):
        m = (rs + 64) % N
        return g[c, m:m + n, POS[t] * B:(POS[t] + 1) * B]

    for side in (UP, DN):
        m = outgoing(
            side,
            lambda rs: jnp.where(low_half, tile(0, rs, 64, 2), roll64(tile(1, rs, 64, 2))),
            own_u,
        )
        for h in range(2):
            s_mid[side, h * 64:h * 64 + 64] = m[h]
        go("gmid", side)
    to_sides(MARGIN)
    go("gcor", LF)
    go("gcor", RT)

    columns_out(INSIDE)
    to_sides(INSIDE)
    for name in GOWN:
        go(name, LF)
        go(name, RT)

    def edges(e):
        arrive("gcor", LF if e == 0 else RT)
        for side in (UP, DN):
            for c in range(2):
                if e == 0:
                    mine = lambda rs: tile(c, rs, 64, 1)
                else:
                    mine = lambda rs: roll64(
                        jnp.where(low_half, tile(c, rs, 64, 3), tile(c, rs, 64, 2))
                    )
                m = outgoing(side, mine, own_u)
                o = outgoing(
                    side,
                    lambda rs: rg[e, c, (rs + 64) % N:(rs + 64) % N + 64],
                    offs[2 * e, 1, 0:1, :],
                )
                for h in range(2):
                    s_edge[side, e, c, h * 64:h * 64 + 64] = m[h] + o[h]
            go("gedge%d" % e, side)

    for which in ("ginner", "gouter"):
        for e in range(2):
            @pl.when(core == (1 - e if which == "ginner" else e))
            def _():
                edges(e)

    pass_on(*GOWN)

    for name in GOWN:
        arrive(name, LF)
        arrive(name, RT)
    lanes = lane_row(OWN)
    for c in range(2):
        x = roll64(rg[1, c, 192:N])
        acc[c, :, 0:B] = light[:, 0:B] * (tile(c, B, OWN, 1) + rg[0, c, 192:N])
        acc[c, :, B:256] = light[:, B:256] * (
            tile(c, B, OWN, 2) + jnp.where(lanes >= 64, x, 0.0)
        )
        acc[c, :, 256:384] = light[:, 256:384] * (tile(c, B, OWN, 3) + x)
        out_ref[c, B:192, :] = acc[c, B:192, 0:OWN]

    for side, rs in ((UP, 0), (DN, 192)):
        arrive("gmid", side)
        arrive("gedge0", side)
        arrive("gedge1", side)
        at = slice(rs, rs + B)
        for c in range(2):
            x = roll64(r_edge[side, 1, c])
            m = r_mid[side] if c == 0 else roll64(r_mid[side])
            out_ref[c, at, 0:B] = acc[c, at, 0:B] + light[at, 0:B] * r_edge[side, 0, c]
            out_ref[c, at, B:256] = acc[c, at, B:256] + light[at, B:256] * jnp.where(
                lane_row(B) < 64, m, x
            )
            last = acc[c, at, 256:384] + light[at, 256:384] * x
            out_ref[c, at, 256:OWN] = last[:, 0:64]

    for (name, direction), (slot, src, dst) in plan.items():
        if name in ("outer", "inner"):
            continue
        if direction in (UP, DN) or name not in RELAYED:
            @pl.when(has[direction])
            def _():
                message(direction, slot, src, dst).wait_send()
            continue
        crossing = col == CROSS[direction - LF]

        @pl.when(has[direction] & jnp.logical_not(crossing))
        def _():
            message(direction, slot, src, dst).wait_send()

        via, first, second = routed(name, direction)

        @pl.when(crossing)
        def _():
            first().wait_send()

        @pl.when(col == via)
        def _():
            second().wait_send()


def local(rows, cols, object_slab, probe_field, offsets, counts):
    hbm = pl.BlockSpec(memory_space=pl.ANY)
    vmem = pltpu.VMEM
    step = pl.pallas_call(
        functools.partial(kernel, rows, cols),
        out_shape=pltpu.VMEM((2, OWN, OWN), F32),
        in_specs=[hbm] * 5,
        out_specs=pl.BlockSpec(memory_space=pltpu.VMEM),
        scratch_shapes=[
            pltpu.SMEM((1, 1, 1, 2), jnp.int32),
            vmem((2, OWN, OWN), F32),
            vmem((2, N, N), F32),
            vmem((N, N), jnp.int32),
            vmem((2, 2, 4, 256, 256), BF16),
            vmem((3, 3, 8, B), F32),
            vmem((2, 2, OWN, B), F32),
            vmem((B, B), F32),
            vmem((B, B), F32),
            vmem((2, 2, 2, B, B), F32),
            vmem((2, B, B), F32),
            vmem((2, 2, OWN, B), F32),
            vmem((2, 2, 2, B, B), F32),
            vmem((2, 2, 160, B), F32),
            vmem((2, N, N), BF16),
            vmem((2, N, N), F32),
            vmem((N, N), F32),
            vmem((OWN, 384), F32),
            vmem((2, N, N), F32),
            vmem((4, 256, N), BF16),
            vmem((4, 256, N), BF16),
            vmem((2, N, N), F32),
            vmem((4, 256, N), F32),
            vmem((4, N, 256), BF16),
            vmem((4, N, 256), BF16),
            vmem((4, N, 256), F32),
            vmem((2, OWN, 384), F32),
            vmem((2, N, N), F32),
            vmem((2, 2, N, B), F32),
            vmem((2, 2, N, B), F32),
            vmem((2, 2, 2, B, B), F32),
            vmem((2, B, B), F32),
            vmem((2, 2, 2, B, B), F32),
            vmem((2, B, B), F32),
            pltpu.SemaphoreType.DMA((5,)),
            pltpu.SemaphoreType.DMA((40,)),
            pltpu.SemaphoreType.DMA((40,)),
        ],
        compiler_params=pltpu.CompilerParams(
            collective_id=0, has_side_effects=True, vmem_limit_bytes=56 * 1024 * 1024
        ),
        name="step",
    )
    return object_slab - step(
        object_slab, probe_field, offsets, counts, jnp.asarray(tables())
    )


def solution(mesh):
    return jax.shard_map(
        functools.partial(local, mesh.shape["row"], mesh.shape["col"]),
        mesh=mesh,
        in_specs=(
            P(None, "row", "col"),
            P(),
            P("row", "col", None, None),
            P("row", "col", None, None, None),
        ),
        out_specs=P(None, "row", "col"),
        check_vma=False,
    )
```

```python
import functools
import math

import jax
import jax.numpy as jnp
import numpy as np
from jax import lax
from jax.experimental import pallas as pl
from jax.experimental.pallas import tpu as pltpu
from jax.sharding import PartitionSpec as P

EPSILON = 0.01
PHOTON_SCALE = 0.01
STEP_SIZE = 0.5
REGULAR = 1.0

N = 512
B = 128
OWN = 320
NOWHERE = -10000.0
F32 = jnp.float32
BF16 = jnp.bfloat16
POS = (1, 2, 3, 0)


def tables():
    k = np.arange(B)[:, None]
    n = np.arange(B)[None, :]
    out = []
    for r in range(4):
        angle = 2.0 * math.pi * (((4 * k + r) * n) % N) / N
        c, s = np.cos(angle) / math.sqrt(N), np.sin(angle) / math.sqrt(N)
        out.append(np.block([[c, s], [-s, c]]))
    full = np.stack(out).astype(np.float32)
    both = np.stack([full, full.transpose(0, 2, 1)])
    high = both.astype(jnp.bfloat16)
    low = (both - high.astype(np.float32)).astype(jnp.bfloat16)
    return np.stack([high, low])


def split(x):
    high = x.astype(BF16)
    return high, (x - high.astype(F32)).astype(BF16)


def dot(a, b):
    return jnp.dot(a, b, preferred_element_type=F32)


def iota(shape, dim):
    return lax.broadcasted_iota(jnp.int32, shape, dim)


def onehot(mask):
    return jnp.where(mask, 1.0, 0.0).astype(BF16)


def roll64(x):
    return pltpu.roll(x, 64, 1)


def kernel(
    rows, cols,
    obj_hbm, probe_hbm, off_hbm, counts_hbm, tab_hbm,
    out_ref,
    off_ref, obj, probe, counts, tab, offs, edge, mid_up, mid_dn,
    in_edge, in_mid, in_own, in_cor, relay_in,
    lum, pp, meas, light, ex, zh, zl, y, back, kh, kl, w, acc, g, sg, rg, s_edge, s_mid, r_edge, r_mid,
    load_sem, send_sem, recv_sem,
):
    row, col = lax.axis_index("row"), lax.axis_index("col")
    core = lax.rem(col, 2)
    has = (row > 0, row < rows - 1, col > 0, col < cols - 1)
    peer = ({"row": row - 1}, {"row": row + 1}, {"col": col - 1}, {"col": col + 1})
    UP, DN, LF, RT = range(4)
    MESH = pl.DeviceIdType.MESH

    def load(src, dst, i):
        return pltpu.make_async_copy(src, dst, load_sem.at[i])

    loads = [
        load(obj_hbm, obj, 0),
        load(probe_hbm, probe, 1),
        load(counts_hbm.at[0, 0, 0], counts, 2),
        load(tab_hbm, tab, 3),
        load(off_hbm, off_ref, 4),
    ]
    loads[0].start()
    loads[4].start()

    barrier = pltpu.get_barrier_semaphore()
    for d in range(4):
        @pl.when(has[d])
        def _():
            pl.semaphore_signal(barrier, inc=1, device_id=peer[d], device_id_type=MESH)

    OPP = (DN, UP, RT, LF)
    CROSS = (8, 7)
    RELAYS = {LF: (3, 1, 5), RT: (13, 15, 11)}
    OWNS, GOWN = ("own0", "own1"), ("gown0", "gown1", "gown2")
    RELAYED = OWNS + ("cor0",) + GOWN
    PARTS = (slice(0, 160), slice(160, OWN))
    GPARTS = (slice(192, 296), slice(296, 400), slice(400, N))
    crossers = [(col == c) for c in CROSS]
    is_relay = functools.reduce(
        jnp.logical_or, [col == c for d in (LF, RT) for c in RELAYS[d]]
    )
    @pl.when(is_relay)
    def _():
        for c in CROSS:
            pl.semaphore_signal(barrier, inc=1, device_id={"col": c}, device_id_type=MESH)

    @pl.when(functools.reduce(jnp.logical_or, crossers))
    def _():
        for c in RELAYS[LF] + RELAYS[RT]:
            pl.semaphore_signal(barrier, inc=1, device_id={"col": c}, device_id_type=MESH)

    def message(direction, slot, src, dst):
        return pltpu.make_async_remote_copy(
            src_ref=src, dst_ref=dst,
            send_sem=send_sem.at[slot], recv_sem=recv_sem.at[slot],
            device_id=peer[direction], device_id_type=MESH,
        )

    def send(direction, slot, src, dst):
        @pl.when(has[direction])
        def _():
            message(direction, slot, src, dst).start()

    plan = {
        ("off", UP): (0, offs.at[1, 1], offs.at[1, 2]),
        ("off", DN): (1, offs.at[1, 1], offs.at[1, 0]),
        ("outer", UP): (2, edge.at[core, :, 0:B], in_edge.at[1, core]),
        ("outer", DN): (3, edge.at[core, :, OWN - B:OWN], in_edge.at[0, core]),
        ("inner", UP): (28, edge.at[1 - core, :, 0:B], in_edge.at[1, 1 - core]),
        ("inner", DN): (29, edge.at[1 - core, :, OWN - B:OWN], in_edge.at[0, 1 - core]),
        ("mid", UP): (4, mid_up, in_mid.at[1]),
        ("mid", DN): (5, mid_dn, in_mid.at[0]),
        ("off", LF): (6, offs.at[1], offs.at[2]),
        ("off", RT): (7, offs.at[1], offs.at[0]),
        **{(OWNS[k], LF): (8 + 2 * k, edge.at[0, :, p], in_own.at[1, :, p]) for k, p in enumerate(PARTS)},
        **{(OWNS[k], RT): (9 + 2 * k, edge.at[1, :, p], in_own.at[0, :, p]) for k, p in enumerate(PARTS)},
        ("cor0", LF): (16, in_edge.at[0, 0], in_cor.at[1, 0]),
        ("cor0", RT): (17, in_edge.at[0, 1], in_cor.at[0, 0]),
        ("cor1", LF): (22, in_edge.at[1, 0], in_cor.at[1, 1]),
        ("cor1", RT): (23, in_edge.at[1, 1], in_cor.at[0, 1]),
        ("gcor", LF): (24, sg.at[0, :, 0:192], rg.at[1, :, 0:192]),
        ("gcor", RT): (25, sg.at[1, :, 0:192], rg.at[0, :, 0:192]),
        **{(GOWN[k], LF): (34 + 2 * k, sg.at[0, :, p], rg.at[1, :, p]) for k, p in enumerate(GPARTS)},
        **{(GOWN[k], RT): (35 + 2 * k, sg.at[1, :, p], rg.at[0, :, p]) for k, p in enumerate(GPARTS)},
        ("gmid", UP): (18, s_mid.at[0], r_mid.at[1]),
        ("gmid", DN): (19, s_mid.at[1], r_mid.at[0]),
        ("gedge0", UP): (20, s_edge.at[0, 0], r_edge.at[1, 0]),
        ("gedge0", DN): (21, s_edge.at[1, 0], r_edge.at[0, 0]),
        ("gedge1", UP): (30, s_edge.at[0, 1], r_edge.at[1, 1]),
        ("gedge1", DN): (31, s_edge.at[1, 1], r_edge.at[0, 1]),
    }

    def routed(name, direction):
        slot, src, dst = plan[name, direction]
        k, phase = 2 if name == "cor0" else int(name[-1]), 0 if name[0] != "g" else 1
        held, held_slot = relay_in.at[phase, :, 0:src.shape[-2]], 26 + phase

        def leg(source, target, sent, received, to):
            return pltpu.make_async_remote_copy(
                src_ref=source, dst_ref=target,
                send_sem=send_sem.at[sent], recv_sem=recv_sem.at[received],
                device_id={"col": to}, device_id_type=MESH,
            )

        via, end = RELAYS[direction][k], CROSS[1 - (direction - LF)]
        return (
            via,
            lambda: leg(src, held, slot, held_slot, via),
            lambda: leg(held, dst, held_slot, slot, end),
        )

    def go(name, direction):
        if direction not in (LF, RT) or name not in RELAYED:
            send(direction, *plan[name, direction])
            return
        crossing = col == CROSS[direction - LF]

        @pl.when(has[direction] & jnp.logical_not(crossing))
        def _():
            message(direction, *plan[name, direction]).start()

        @pl.when(crossing)
        def _():
            routed(name, direction)[1]().start()

    def gone(name, direction):
        @pl.when(has[direction])
        def _():
            message(direction, *plan[name, direction]).wait_send()

    def pass_on(*names):
        for name in names:
            for direction in (LF, RT):
                via, first, second = routed(name, direction)

                @pl.when(col == via)
                def _():
                    first().wait_recv()
                    second().start()

    def arrive(name, side):
        slot, src, dst = plan[name, OPP[side]]

        @pl.when(has[side])
        def _():
            message(side, slot, src, dst).wait_recv()

    def corner(which, side):
        arrive(which, side)
        left = core if which == "inner" else 1 - core
        for direction, flag in ((LF, 1), (RT, 0)):
            @pl.when(left == flag)
            def _():
                go("cor%d" % side, direction)

    lane_row = lambda n: iota((n, B), 1)
    low_half = lane_row(64) < 64

    @pl.when(row == 0)
    def _():
        in_edge[0] = jnp.zeros(in_edge.shape[1:], F32)
        in_mid[0] = jnp.zeros(in_mid.shape[1:], F32)
        r_edge[0] = jnp.zeros(r_edge.shape[1:], F32)
        r_mid[0] = jnp.zeros(r_mid.shape[1:], F32)
        offs[1, 0] = jnp.full((8, B), NOWHERE, F32)

    @pl.when(row == rows - 1)
    def _():
        in_edge[1] = jnp.zeros(in_edge.shape[1:], F32)
        in_mid[1] = jnp.zeros(in_mid.shape[1:], F32)
        r_edge[1] = jnp.zeros(r_edge.shape[1:], F32)
        r_mid[1] = jnp.zeros(r_mid.shape[1:], F32)
        offs[1, 2] = jnp.full((8, B), NOWHERE, F32)

    @pl.when(col == 0)
    def _():
        in_own[0] = jnp.zeros(in_own.shape[1:], F32)
        in_cor[0] = jnp.zeros(in_cor.shape[1:], F32)
        rg[0] = jnp.zeros(rg.shape[1:], F32)
        offs[0] = jnp.full((3, 8, B), NOWHERE, F32)

    @pl.when(col == cols - 1)
    def _():
        in_own[1] = jnp.zeros(in_own.shape[1:], F32)
        in_cor[1] = jnp.zeros(in_cor.shape[1:], F32)
        rg[1] = jnp.zeros(rg.shape[1:], F32)
        offs[2] = jnp.full((3, 8, B), NOWHERE, F32)

    loads[4].wait()
    u, v = off_ref[0, 0, 0, 0], off_ref[0, 0, 0, 1]
    uf, vf = u.astype(F32), v.astype(F32)
    offs[1, 1] = jnp.where(iota((8, B), 0) == 0, uf, vf)

    loads[0].wait()
    for c in loads[1:4]:
        c.start()
    def tail(rs, n, ch):
        x = obj[ch, rs:rs + n, 256:OWN]
        return jnp.concatenate([x, x], axis=1)

    for ch in range(2):
        edge[0, ch] = obj[ch, :, 0:B]
        edge[1, ch] = jnp.where(
            lane_row(OWN) < 64, roll64(obj[ch, :, B:256]), tail(0, OWN, ch)
        )
    for ref, rs in ((mid_up, 0), (mid_dn, OWN - B)):
        ref[...] = jnp.where(
            lane_row(B) < 64, obj[0, rs:rs + B, B:256], roll64(obj[1, rs:rs + B, B:256])
        )

    pl.semaphore_wait(
        barrier,
        sum(h.astype(jnp.int32) for h in has)
        + 2 * is_relay.astype(jnp.int32)
        + 6 * sum(c.astype(jnp.int32) for c in crossers),
    )

    for name in ("off", "outer"):
        go(name, UP)
        go(name, DN)
    for name in OWNS:
        go(name, LF)
        go(name, RT)

    loads[1].wait()
    for q in range(4):
        rs = slice(q * B, (q + 1) * B)
        pr, pi = probe[0, rs], probe[1, rs]
        hi, lo = split(pr * pr + pi * pi)
        lum[0, rs] = hi
        lum[1, rs] = lo
    d = iota((N, N), 0) + v - ((iota((N, N), 1) + 3 * B) % N)
    right = onehot((d == 0) | (d == N))
    d = iota((N, N), 1) + u - (iota((N, N), 0) + 448) % N
    left = onehot((d == 0) | (d == N))
    for ch in range(2):
        hi, lo = split(probe[ch])
        hi, lo = split(dot(hi, right) + dot(lo, right))
        pp[ch] = dot(left, hi) + dot(left, lo)

    arrive("off", UP)
    arrive("off", DN)
    go("off", LF)
    go("off", RT)

    loads[2].wait()
    a, b = iota((N, N), 0), iota((N, N), 1)
    order_right = onehot(a == (b % B) * 4 + b // B)
    order_left = onehot(b == (a % B) * 4 + a // B)
    hi, lo = split(counts[...].astype(F32))
    hi, lo = split(dot(hi, order_right) + dot(lo, order_right))
    meas[...] = jnp.sqrt((dot(order_left, hi) + dot(order_left, lo)) * PHOTON_SCALE)

    for direction in (UP, DN):
        gone("outer", direction)
    go("inner", UP)
    go("inner", DN)
    corner("outer", UP)

    arrive("off", LF)
    arrive("off", RT)
    light[...] = jnp.zeros(light.shape, F32)
    row_of = ((0, B, 384, B, 448), (0, OWN, 0, N, 128), (192, B, 0, B, -192))
    col_of = ((0, B, 384, B, 448), (0, 384, 0, N, 128), (128, 256, 0, B, -192))

    def tiled(x, n):
        return x if n == B else jnp.concatenate([x] * (n // B), axis=1)

    for dc in range(3):
        c0, cn, j0, jn, cshift = col_of[dc]
        for dr in range(3):
            r0, rn, i0, im, rshift = row_of[dr]
            ou = tiled(offs[dc, dr, 0:1, :], im)
            ov = tiled(offs[dc, dr, 1:2, :], cn)
            i_row = (iota((rn, im), 1) + (i0 - r0 - rshift) - iota((rn, im), 0)).astype(F32)
            pick_row = onehot(i_row + ou == 0.0)
            i_col = (iota((jn, cn), 0) + (j0 - c0 - cshift) - iota((jn, cn), 1)).astype(F32)
            pick_col = onehot(i_col + ov == 0.0)
            part = sum(dot(pick_row, lum[h, i0:i0 + im, j0:j0 + jn]) for h in range(2))
            hi, lo = split(part)
            light[r0:r0 + rn, c0:c0 + cn] += dot(hi, pick_col) + dot(lo, pick_col)
    light[...] = STEP_SIZE / (light[...] + REGULAR)

    pass_on(*OWNS)

    def fwd4(x):
        (ar, ai), (br, bi), (cr, ci), (dr_, di) = x
        er, ei, fr, fi = ar + cr, ai + ci, ar - cr, ai - ci
        gr, gi, hr, hi_ = br + dr_, bi + di, br - dr_, bi - di
        return [
            (er + gr, ei + gi), (fr + hi_, fi - hr),
            (er - gr, ei - gi), (fr - hi_, fi + hr),
        ]

    def inv4(x):
        (ar, ai), (br, bi), (cr, ci), (dr_, di) = x
        er, ei, fr, fi = ar + cr, ai + ci, ar - cr, ai - ci
        gr, gi, hr, hi_ = br + dr_, bi + di, br - dr_, bi - di
        return [
            (er + gr, ei + gi), (fr - hi_, fi + hr),
            (er - gr, ei - gi), (fr + hi_, fi - hr),
        ]

    def dot3(a_hi, a_lo, b_hi, b_lo):
        return dot(a_hi, b_hi) + dot(a_hi, b_lo) + dot(a_lo, b_hi)

    def columns_in(rs):
        z = fwd4([
            tuple(ex[c, rs, POS[q] * B:(POS[q] + 1) * B] for c in range(2)) for q in range(4)
        ])
        for f in range(4):
            for c in range(2):
                hi, lo = split(z[f][c])
                kh[f, rs, c * B:(c + 1) * B] = hi
                kl[f, rs, c * B:(c + 1) * B] = lo
        for f in range(4):
            out = dot3(kh[f, rs], kl[f, rs], tab[0, 1, f], tab[1, 1, f])
            for c in range(2):
                y[c, rs, f * B:(f + 1) * B] = out[:, c * B:(c + 1) * B]

    def columns_out(rs):
        for f in range(4):
            w[f, rs] = dot3(kh[f, rs], kl[f, rs], tab[0, 0, f], tab[1, 0, f])
        x = inv4([(w[f, rs, 0:B], w[f, rs, B:256]) for f in range(4)])
        for q in range(4):
            ls = slice(POS[q] * B, (POS[q] + 1) * B)
            pr, pi = pp[0, rs, ls], pp[1, rs, ls]
            br, bi = x[q]
            g[0, rs, ls] = pr * br + pi * bi
            g[1, rs, ls] = pr * bi - pi * br

    MARGIN, INSIDE = slice(0, 192), slice(192, N)

    def put(rs, n, t, wr, wi):
        m = (rs + 64) % N
        at = (slice(m, m + n), slice(POS[t] * B, (POS[t] + 1) * B))
        pr, pi = pp[(0,) + at], pp[(1,) + at]
        ex[(0,) + at] = pr * wr - pi * wi
        ex[(1,) + at] = pr * wi + pi * wr

    put(B, OWN, 1, obj[0, :, 0:B], obj[1, :, 0:B])
    put(B, OWN, 2, obj[0, :, B:256], obj[1, :, B:256])

    def side_tiles(rs, n, ends, from_left, from_right):
        half = lane_row(n) < 64
        back = [roll64(x) for x in from_right]
        put(rs, n, 3, *(jnp.where(half, e, x) for e, x in zip(ends, back)))
        put(rs, n, 0, *(jnp.where(lane_row(n) < v, x, y_) for x, y_ in zip(back, from_left)))

    loads[3].wait()
    corner("outer", DN)
    for direction in (UP, DN):
        gone("inner", direction)
    go("mid", UP)
    go("mid", DN)
    pass_on("cor0")
    corner("inner", UP)
    corner("inner", DN)
    for name in OWNS:
        arrive(name, LF)
        arrive(name, RT)
    side_tiles(
        B, OWN, [tail(0, OWN, ch) for ch in range(2)],
        [in_own[0, ch] for ch in range(2)], [in_own[1, ch] for ch in range(2)],
    )
    columns_in(INSIDE)

    groups = (0, 64, 448)
    row64 = iota((64, B), 0)

    def halo(group, get):
        if group == 0:
            return jnp.where(row64 < u, get(1, 64), get(0, 0))
        if group == 64:
            return get(0, 64)
        return get(1, 0)

    def rolled_edge(group, ch):
        return roll64(halo(group, lambda s, r: in_edge[s, 1, ch, r:r + 64]))

    for rs in groups:
        put(rs, 64, 1, *(halo(rs, lambda s, r: in_edge[s, 0, ch, r:r + 64]) for ch in range(2)))
    for side in (UP, DN):
        arrive("cor%d" % side, LF)
        arrive("cor%d" % side, RT)
    for rs in groups:
        side_tiles(
            rs, 64, [rolled_edge(rs, ch) for ch in range(2)],
            [halo(rs, lambda s, r: in_cor[0, s, ch, r:r + 64]) for ch in range(2)],
            [halo(rs, lambda s, r: in_cor[1, s, ch, r:r + 64]) for ch in range(2)],
        )
    arrive("mid", UP)
    arrive("mid", DN)
    for rs in groups:
        m = halo(rs, lambda s, r: in_mid[s, r:r + 64])
        put(rs, 64, 2, *(
            jnp.where(low_half, m if ch == 0 else roll64(m), rolled_edge(rs, ch))
            for ch in range(2)
        ))
    columns_in(MARGIN)

    def block(ref, c, q):
        if q < 3:
            return ref[c, 64 + q * B:64 + (q + 1) * B]
        return jnp.concatenate([ref[c, 448:N], ref[c, 0:64]], axis=0)

    z = fwd4([tuple(block(y, c, q) for c in range(2)) for q in range(4)])
    for r in range(4):
        for c in range(2):
            hi, lo = split(z[r][c])
            zh[r, c * B:(c + 1) * B] = hi
            zl[r, c * B:(c + 1) * B] = lo
    for r in range(4):
        far = dot3(tab[0, 0, r], tab[1, 0, r], zh[r], zl[r])
        fr, fi = far[0:B], far[B:256]
        factor = 1.0 - meas[r * B:(r + 1) * B] * lax.rsqrt(fr * fr + fi * fi + EPSILON)
        hi, lo = split(jnp.concatenate([factor * fr, factor * fi], axis=0))
        back[r] = dot3(tab[0, 1, r], tab[1, 1, r], hi, lo)
    x = inv4([(back[r, 0:B], back[r, B:256]) for r in range(4)])
    for q in range(4):
        for c in range(2):
            parts = split(x[q][c])
            for f in range(4):
                for ref, part in zip((kh, kl), parts):
                    piece = part[:, f * B:(f + 1) * B]
                    at = slice(c * B, (c + 1) * B)
                    if q < 3:
                        ref[f, 64 + q * B:64 + (q + 1) * B, at] = piece
                    else:
                        ref[f, 448:N, at] = piece[0:64]
                        ref[f, 0:64, at] = piece[64:B]

    def to_sides(rs):
        lanes = lane_row(rs.stop - rs.start)
        inner = lanes < v
        for c in range(2):
            g3, g0 = g[c, rs, 0:B], g[c, rs, B:256]
            sg[0, c, rs] = jnp.where(inner, 0.0, g0)
            sg[1, c, rs] = roll64(jnp.where(lanes >= 64, g3, jnp.where(inner, g0, 0.0)))

    columns_out(MARGIN)

    row64f = row64.astype(F32)

    def outgoing(side, get, ou):
        if side == UP:
            return (jnp.where(row64f >= ou, get(0), 0.0), get(64))
        return (get(448), jnp.where(row64f < ou, get(0), 0.0))

    own_u = offs[1, 1, 0:1, :]

    def tile(c, rs, n, t):
        m = (rs + 64) % N
        return g[c, m:m + n, POS[t] * B:(POS[t] + 1) * B]

    for side in (UP, DN):
        m = outgoing(
            side,
            lambda rs: jnp.where(low_half, tile(0, rs, 64, 2), roll64(tile(1, rs, 64, 2))),
            own_u,
        )
        for h in range(2):
            s_mid[side, h * 64:h * 64 + 64] = m[h]
        go("gmid", side)
    to_sides(MARGIN)
    go("gcor", LF)
    go("gcor", RT)

    def edges(e):
        arrive("gcor", LF if e == 0 else RT)
        for side in (UP, DN):
            for c in range(2):
                if e == 0:
                    mine = lambda rs: tile(c, rs, 64, 1)
                else:
                    mine = lambda rs: roll64(
                        jnp.where(low_half, tile(c, rs, 64, 3), tile(c, rs, 64, 2))
                    )
                m = outgoing(side, mine, own_u)
                o = outgoing(
                    side,
                    lambda rs: rg[e, c, (rs + 64) % N:(rs + 64) % N + 64],
                    offs[2 * e, 1, 0:1, :],
                )
                for h in range(2):
                    s_edge[side, e, c, h * 64:h * 64 + 64] = m[h] + o[h]
            go("gedge%d" % e, side)

    for which in ("ginner", "gouter"):
        if which == "gouter":
            columns_out(INSIDE)
            to_sides(INSIDE)
            for name in GOWN:
                go(name, LF)
                go(name, RT)
        for e in range(2):
            @pl.when(core == (1 - e if which == "ginner" else e))
            def _():
                edges(e)

    pass_on(*GOWN)

    for name in GOWN:
        arrive(name, LF)
        arrive(name, RT)
    lanes = lane_row(OWN)
    for c in range(2):
        x = roll64(rg[1, c, 192:N])
        acc[c, :, 0:B] = light[:, 0:B] * (tile(c, B, OWN, 1) + rg[0, c, 192:N])
        acc[c, :, B:256] = light[:, B:256] * (
            tile(c, B, OWN, 2) + jnp.where(lanes >= 64, x, 0.0)
        )
        acc[c, :, 256:384] = light[:, 256:384] * (tile(c, B, OWN, 3) + x)
        out_ref[c, B:192, :] = acc[c, B:192, 0:OWN]

    for side, rs in ((UP, 0), (DN, 192)):
        arrive("gmid", side)
        arrive("gedge0", side)
        arrive("gedge1", side)
        at = slice(rs, rs + B)
        for c in range(2):
            x = roll64(r_edge[side, 1, c])
            m = r_mid[side] if c == 0 else roll64(r_mid[side])
            out_ref[c, at, 0:B] = acc[c, at, 0:B] + light[at, 0:B] * r_edge[side, 0, c]
            out_ref[c, at, B:256] = acc[c, at, B:256] + light[at, B:256] * jnp.where(
                lane_row(B) < 64, m, x
            )
            last = acc[c, at, 256:384] + light[at, 256:384] * x
            out_ref[c, at, 256:OWN] = last[:, 0:64]

    for (name, direction), (slot, src, dst) in plan.items():
        if name in ("outer", "inner"):
            continue
        if direction in (UP, DN) or name not in RELAYED:
            @pl.when(has[direction])
            def _():
                message(direction, slot, src, dst).wait_send()
            continue
        crossing = col == CROSS[direction - LF]

        @pl.when(has[direction] & jnp.logical_not(crossing))
        def _():
            message(direction, slot, src, dst).wait_send()

        via, first, second = routed(name, direction)

        @pl.when(crossing)
        def _():
            first().wait_send()

        @pl.when(col == via)
        def _():
            second().wait_send()


def local(rows, cols, object_slab, probe_field, offsets, counts):
    hbm = pl.BlockSpec(memory_space=pl.ANY)
    vmem = pltpu.VMEM
    step = pl.pallas_call(
        functools.partial(kernel, rows, cols),
        out_shape=pltpu.VMEM((2, OWN, OWN), F32),
        in_specs=[hbm] * 5,
        out_specs=pl.BlockSpec(memory_space=pltpu.VMEM),
        scratch_shapes=[
            pltpu.SMEM((1, 1, 1, 2), jnp.int32),
            vmem((2, OWN, OWN), F32),
            vmem((2, N, N), F32),
            vmem((N, N), jnp.int32),
            vmem((2, 2, 4, 256, 256), BF16),
            vmem((3, 3, 8, B), F32),
            vmem((2, 2, OWN, B), F32),
            vmem((B, B), F32),
            vmem((B, B), F32),
            vmem((2, 2, 2, B, B), F32),
            vmem((2, B, B), F32),
            vmem((2, 2, OWN, B), F32),
            vmem((2, 2, 2, B, B), F32),
            vmem((2, 2, 160, B), F32),
            vmem((2, N, N), BF16),
            vmem((2, N, N), F32),
            vmem((N, N), F32),
            vmem((OWN, 384), F32),
            vmem((2, N, N), F32),
            vmem((4, 256, N), BF16),
            vmem((4, 256, N), BF16),
            vmem((2, N, N), F32),
            vmem((4, 256, N), F32),
            vmem((4, N, 256), BF16),
            vmem((4, N, 256), BF16),
            vmem((4, N, 256), F32),
            vmem((2, OWN, 384), F32),
            vmem((2, N, N), F32),
            vmem((2, 2, N, B), F32),
            vmem((2, 2, N, B), F32),
            vmem((2, 2, 2, B, B), F32),
            vmem((2, B, B), F32),
            vmem((2, 2, 2, B, B), F32),
            vmem((2, B, B), F32),
            pltpu.SemaphoreType.DMA((5,)),
            pltpu.SemaphoreType.DMA((40,)),
            pltpu.SemaphoreType.DMA((40,)),
        ],
        compiler_params=pltpu.CompilerParams(
            collective_id=0, has_side_effects=True, vmem_limit_bytes=56 * 1024 * 1024
        ),
        name="step",
    )
    return object_slab - step(
        object_slab, probe_field, offsets, counts, jnp.asarray(tables())
    )


def solution(mesh):
    return jax.shard_map(
        functools.partial(local, mesh.shape["row"], mesh.shape["col"]),
        mesh=mesh,
        in_specs=(
            P(None, "row", "col"),
            P(),
            P("row", "col", None, None),
            P("row", "col", None, None, None),
        ),
        out_specs=P(None, "row", "col"),
        check_vma=False,
    )
```
